32 devices in a mesh: group: 8 (over y, x, core), tile: 4 (over z).
Axes of the slice: x: 2, y: 2, z: 4, core: 2. Of those that a mesh axis runs over, the one named last changes fastest.
Arguments:
- coupling: float32 [32, 1024, 768], P('group', None, 'tile'), may hold values from -6 to 6
- interior_solve: float32 [32, 768, 1024], P('group', 'tile'), may hold values from -0.21875 to 0.21875
- boundary_stiffness: float32 [32, 1024, 1024], P('group', 'tile'), may hold values from -6 to 6
- migration: int32 [32], replicated, may hold values from -1 to 15, as said below
Outputs:
- condensed: float32 [16, 1024, 1024], P('group', 'tile')
The draws below stay inside these ranges and needn't reach their ends.
Inputs may be any that keep to these rules, and one draw needn't show every extreme that they name: `migration`: every condensed slot is named by exactly one RVE slot; RVE slots of group g are g * 4 to g * 4 + 3; the condensed slots of group g are named only by RVE slots of group g or of its partner, the group whose index differs from g in the lowest bit; some group holds 4 plastic RVEs.
All inputs are finite; a program needn't handle non-finite values.
Results may differ from the reference program's by a relative error of at most 0.000071.
Values sent between devices are 32-bit elements; how exact they have to be, the bound alone decides.
A program may use at most 64 MiB of HBM per device.

```python
import jax
import jax.numpy as jnp
from jax import lax

BOUNDARY = 1024
INTERIOR = 768
OWN = 2
HOME = 4
RVES = 32
SLOTS = 16


def draw_migration(key, part):
    groups = RVES // HOME
    couples = groups // 2
    key_heavy, key_slots = jax.random.split(jax.random.fold_in(key, 23))
    heavy_bit = jax.random.randint(key_heavy, (couples,), 0, 2).astype(jnp.int32)
    couple_ids = jnp.arange(couples, dtype=jnp.int32)
    heavies = 2 * couple_ids + heavy_bit
    lights = 2 * couple_ids + 1 - heavy_bit
    slot_ids = jnp.arange(OWN, dtype=jnp.int32)[None, :]
    targets = jnp.concatenate([heavies[:, None] * OWN + slot_ids, lights[:, None] * OWN + slot_ids], axis=1)
    subkeys = jax.random.split(key_slots, couples)
    shuffles = jax.vmap(lambda sub_key: jax.random.permutation(sub_key, HOME))(subkeys).astype(jnp.int32)
    places = heavies[:, None] * HOME + shuffles
    result = jnp.full((RVES,), -1, jnp.int32)
    return result.at[places.reshape(-1)].set(targets.reshape(-1).astype(jnp.int32))


def block_scale(key, extent, shards, least, largest):
    level = 1.0
    for dim, parts in shards:
        steps = jax.random.uniform(jax.random.fold_in(jax.random.fold_in(key, 6), dim), (parts,), jnp.float32, least / len(shards), largest / len(shards))
        level = level * jnp.repeat(jnp.exp(steps), extent[dim] // parts).reshape((-1,) + (1,) * (len(extent) - 1 - dim))
    return level


def scatter_about(rng, dims, spread, bound, cuts=(), kind=jnp.bfloat16):
    drawn = spread * jax.random.normal(rng, dims, jnp.float32)
    if cuts:
        drawn = drawn * block_scale(rng, dims, cuts, -0.22, 0.18)
    return jnp.clip(drawn, -bound, bound).astype(kind)


def setup_inputs(seed: int = 0) -> dict:
    arg_keys = jax.random.split(jax.random.key(seed), 5)
    return {
        "coupling": scatter_about(arg_keys[0], (RVES, BOUNDARY, INTERIOR), 1.0, 6.0, ((0, 8), (2, 4)), jnp.float32),
        "interior_solve": scatter_about(arg_keys[1], (RVES, INTERIOR, BOUNDARY), INTERIOR ** -0.5, 0.21875, ((0, 8), (1, 4)), jnp.float32),
        "boundary_stiffness": scatter_about(arg_keys[2], (RVES, BOUNDARY, BOUNDARY), 1.0, 6.0, ((0, 8), (1, 4)), jnp.float32),
        "migration": draw_migration(jax.random.fold_in(arg_keys[4], 71), 0),
    }


def reference(coupling, interior_solve, boundary_stiffness, migration):
    targets = jnp.where(migration >= 0, migration, SLOTS).astype(jnp.int32)
    sources = jnp.zeros((SLOTS,), jnp.int32).at[targets].set(jnp.arange(RVES, dtype=jnp.int32), mode="drop")

    def condense_one(source):
        product = jnp.dot(coupling[source], interior_solve[source], precision=lax.Precision.HIGHEST, preferred_element_type=jnp.float32)
        return boundary_stiffness[source] - product

    return lax.map(condense_one, sources)
```

```python
import jax
import jax.numpy as jnp
from jax import lax
from jax.experimental import pallas as pl
from jax.experimental.pallas import tpu as pltpu
from jax.sharding import PartitionSpec as P

OWN = 2


def swapped(array, axis, distance):
    return lax.ppermute(array, axis, [(i, i ^ 1 << distance) for i in range(lax.axis_size(axis))])


def condense(coupling_cols, solve_rows, stiff_rows):
    product = lax.psum_scatter(
        jnp.dot(
            coupling_cols,
            solve_rows,
            precision=lax.Precision.HIGHEST,
            preferred_element_type=jnp.float32,
        ),
        "tile",
        scatter_dimension=0,
        tiled=True,
    )
    return stiff_rows - product


def select_slots(stacked, positions, present):
    chosen = jnp.take(stacked, positions, axis=0)
    shaped = present.reshape((-1,) + (1,) * (stacked.ndim - 1))
    return jnp.where(shaped, chosen, jnp.zeros_like(chosen))


def portable_body(coupling, interior_solve, boundary_stiffness, migration):
    home_count = coupling.shape[0]
    mygroup = lax.axis_index("group")
    partner = jnp.bitwise_xor(mygroup, 1)
    own_plan = lax.dynamic_slice_in_dim(migration, mygroup * home_count, home_count)
    slot_ids = jnp.arange(OWN, dtype=jnp.int32)
    local_ids = jnp.arange(home_count, dtype=jnp.int32)

    def locate(wanted):
        matches = own_plan[None, :] == wanted[:, None]
        positions = jnp.sum(jnp.where(matches, local_ids[None, :], 0), axis=1)
        return (positions, jnp.any(matches, axis=1))

    mine_index, mine_here = locate(mygroup * OWN + slot_ids)
    their_index, their_here = locate(partner * OWN + slot_ids)
    keep_mask = mine_here[:, None, None]
    outgoing = (
        select_slots(coupling, their_index, their_here),
        select_slots(interior_solve, their_index, their_here),
        select_slots(boundary_stiffness, their_index, their_here),
    )
    arrived = swapped((outgoing[0], outgoing[1], outgoing[2]), "group", 0)
    kept_coupling = jnp.where(keep_mask, jnp.take(coupling, mine_index, axis=0), arrived[0])
    kept_solve = jnp.where(keep_mask, jnp.take(interior_solve, mine_index, axis=0), arrived[1])
    kept_stiff = jnp.where(keep_mask, jnp.take(boundary_stiffness, mine_index, axis=0), arrived[2])
    result = jnp.stack(
        [condense(kept_coupling[slot], kept_solve[slot], kept_stiff[slot]) for slot in range(OWN)]
    )
    return result


MESH = pl.DeviceIdType.MESH
LINE = 4
CHUNKS = 4
STRIP = 64
AHEAD = 3
K, X, B = 0, 1, 2
PIECES = ((K, 0), (X, 0), (K, 1), (X, 1), (X, 2), (X, 3), (K, 2), (K, 3))
FED = 7
FAR = 6


def split_into(stack, base, depth, rows, value, order):
    high = value.astype(jnp.bfloat16)
    low = (value - high.astype(jnp.float32)).astype(jnp.bfloat16)
    for place, term in enumerate(order):
        stack[pl.ds(base + place * depth + rows, value.shape[0]), :] = high if term == 0 else low


def contract(left, right):
    return lax.dot_general(left, right, (((0,), (0,)), ((), ())), preferred_element_type=jnp.float32)


def strips(count, body):
    @pl.loop(0, count // STRIP)
    def _(i):
        body(pl.multiple_of(i * STRIP, STRIP))


def line_kernel(
    plan, k_hbm, x_hbm, b_hbm, result,
    k_home0, k_home1, k_home2, k_home3, x_home0, x_home1, x_home2, x_home3, b_home,
    k_out, x_out, b_out, k_in, x_in, b_in, k_got, x_got,
    k_end, x_end, k_far, x_far, k_stack, x_stack, kf_stack, xf_stack, p_send, p_recv, e_send, e_recv,
    load_sem, mig_send, mig_recv, em_send, em_recv, far_send, far_recv, mm_send, mm_recv, me_send, me_recv,
):
    homes = ((k_home0, k_home1, k_home2, k_home3), (x_home0, x_home1, x_home2, x_home3))
    home, depth = k_home0.shape[:2]
    rows = b_home.shape[1]
    width = x_home0.shape[2]
    last = LINE - 1
    g, t = lax.axis_index("group"), lax.axis_index("tile")
    parity = g % 2
    partner = g + 1 - 2 * parity
    side = t // 2
    end, mid = side * last, 1 + side
    far_end, across = last - end, last - mid
    is_end = t == end
    is_mid = t == mid
    even_mid = is_mid & (parity == 0)
    odd_mid = is_mid & (parity == 1)

    def chunk(index):
        return pl.ds(pl.multiple_of(index * width, width), width)

    def load(q):
        kind, n = PIECES[q]
        at = chunk(n) if kind == X else pl.ds(pl.multiple_of((far_end, across, mid, end)[n] * rows, rows), rows)
        return pltpu.make_async_copy((k_hbm, x_hbm)[kind].at[:, :, at], homes[kind][n], load_sem.at[q])

    b_load = pltpu.make_async_copy(b_hbm, b_home, load_sem.at[len(PIECES)])
    for q in range(AHEAD):
        load(q).start()

    barrier = pltpu.get_barrier_semaphore()
    pl.semaphore_signal(barrier, inc=1, device_id=(partner, t), device_id_type=MESH)

    @pl.when(is_end)
    def _():
        pl.semaphore_signal(barrier, inc=1, device_id=(g, mid), device_id_type=MESH)

    @pl.when(is_mid)
    def _():
        pl.semaphore_signal(barrier, inc=1, device_id=(g, end), device_id_type=MESH)
        pl.semaphore_signal(barrier, inc=1, device_id=(g, across), device_id_type=MESH)

    def find(wanted):
        index, here = jnp.int32(0), jnp.int32(0)
        for j in range(home):
            hit = plan[g * home + j] == wanted
            index, here = jnp.where(hit, j, index), jnp.where(hit, 1, here)
        return index, here > 0

    mine = [find(g * OWN + s) for s in range(OWN)]
    theirs = [find(partner * OWN + s) for s in range(OWN)]

    def migrate(q, s):
        if q == len(PIECES):
            src, dst = b_out.at[s], b_in.at[s]
        else:
            kind, n = PIECES[q]
            src, dst = (k_out, x_out)[kind].at[s, n], (k_in, x_in)[kind].at[s, n]
        return pltpu.make_async_remote_copy(
            src_ref=src, dst_ref=dst, send_sem=mig_send.at[s, q], recv_sem=mig_recv.at[s, q],
            device_id=(partner, t), device_id_type=MESH,
        )

    def feed(s, q):
        kind, n = PIECES[q]
        return pltpu.make_async_remote_copy(
            src_ref=(k_got, x_got)[kind].at[s, n], dst_ref=(k_end, x_end)[kind].at[s, n],
            send_sem=em_send.at[s, q], recv_sem=em_recv.at[s, q], device_id=(g, mid), device_id_type=MESH,
        )

    def far(source, q):
        kind, n = PIECES[q]
        src = ((k_got, x_got), (k_end, x_end))[source][kind].at[0, n]
        return pltpu.make_async_remote_copy(
            src_ref=src, dst_ref=(k_far, x_far)[kind].at[source, n],
            send_sem=far_send.at[source, q], recv_sem=far_recv.at[source, q],
            device_id=(g, across), device_id_type=MESH,
        )

    def cross(s, j, c):
        return pltpu.make_async_remote_copy(
            src_ref=p_send.at[s, j, c], dst_ref=p_recv.at[s, j, c],
            send_sem=mm_send.at[s, j, c], recv_sem=mm_recv.at[s, j, c],
            device_id=(g, across), device_id_type=MESH,
        )

    def deliver(s, c, to):
        return pltpu.make_async_remote_copy(
            src_ref=e_send.at[s, c], dst_ref=e_recv.at[s, c],
            send_sem=me_send.at[s, c], recv_sem=me_recv.at[s, c],
            device_id=(g, to), device_id_type=MESH,
        )

    def give(q):
        kind, n = PIECES[q]
        for s in range(OWN):
            def copy(first):
                at = pl.ds(first, STRIP)
                (k_out, x_out)[kind][s, n, at, :] = homes[kind][n][theirs[s][0], at, :]

            strips(depth, copy)
            migrate(q, s).start()

    def settle(q):
        kind, n = PIECES[q]
        for s in range(OWN):
            migrate(q, s).wait_recv()
            index, here = mine[s]

            def choose(first):
                at = pl.ds(first, STRIP)
                (k_got, x_got)[kind][s, n, at, :] = jnp.where(
                    here, homes[kind][n][index, at, :], (k_in, x_in)[kind][s, n, at, :]
                )

            strips(depth, choose)
            if s == 0 and q < FED:
                @pl.when(is_end)
                def _():
                    feed(0, q).start()

            if s == 0 and q < FAR:
                @pl.when(even_mid)
                def _():
                    far(0, q).start()

    for q in range(len(PIECES)):
        load(q).wait()
        if q + AHEAD < len(PIECES):
            load(q + AHEAD).start()
        elif q + AHEAD == len(PIECES):
            b_load.start()
        if q == 0:
            @pl.when(is_end)
            def _():
                pl.semaphore_wait(barrier, 2)

            @pl.when(is_mid)
            def _():
                pl.semaphore_wait(barrier, 3)

        give(q)
        if q > 0:
            settle(q - 1)
    settle(len(PIECES) - 1)

    @pl.when(is_end)
    def _():
        for q in range(FED):
            feed(1, q).start()

    b_load.wait()
    for s in range(OWN):
        def copy(first):
            at = pl.ds(first, STRIP)
            b_out[s, at, :] = b_home[theirs[s][0], at, :]

        strips(rows, copy)
        migrate(len(PIECES), s).start()

    def stack_piece(s, kind, n):
        got, stack, order = ((k_got, k_stack, (0, 0, 1)), (x_got, x_stack, (0, 1, 0)))[kind]
        strips(depth, lambda first: split_into(
            stack.at[s, n], 0, depth, first, got[s, n, pl.ds(first, STRIP), :], order
        ))

    def stiffness(s, c):
        index, here = mine[s]
        return jnp.where(here, b_home[index, :, chunk(c)], b_in[s, :, chunk(c)])

    own_terms = pl.ds(0, 3 * depth)

    @pl.when(is_end)
    def _():
        for s in range(OWN):
            stack_piece(s, K, 3)
            for c in range(CHUNKS):
                stack_piece(s, X, c)
        for s in range(OWN):
            migrate(len(PIECES), s).wait_recv()

            @pl.loop(0, CHUNKS)
            def _(c):
                result[s, :, chunk(c)] = stiffness(s, c) - contract(k_stack[s, 3, own_terms, :], x_stack[s, c, own_terms, :])

        for s in range(OWN):
            @pl.loop(0, CHUNKS)
            def _(c):
                deliver(s, c, mid).wait_recv()
                result[s, :, chunk(c)] = result[s, :, chunk(c)] - e_recv[s, c]

        for s in range(OWN):
            for q in range(FED):
                feed(s, q).wait_send()

    def arrived(s, q):
        kind, n = PIECES[q]
        buffer = (k_end, x_end)[kind].at[s, n]
        pltpu.make_async_remote_copy(
            src_ref=buffer, dst_ref=buffer, send_sem=em_send.at[s, q], recv_sem=em_recv.at[s, q],
            device_id=(g, end), device_id_type=MESH,
        ).wait_recv()

    def stack_arrived(s, q):
        kind, n = PIECES[q]
        got, stack, order = ((k_end, k_stack, (0, 0, 1)), (x_end, x_stack, (0, 1, 0)))[kind]
        strips(depth, lambda first: split_into(
            stack.at[s, n], 3 * depth, depth, first, got[s, n, pl.ds(first, STRIP), :], order
        ))

    def stack_far(source, q):
        kind, n = PIECES[q]
        got, stack, order = ((k_far, kf_stack, (0, 0, 1)), (x_far, xf_stack, (0, 1, 0)))[kind]
        strips(depth, lambda first: split_into(
            stack.at[n], 3 * source * depth, depth, first, got[source, n, pl.ds(first, STRIP), :], order
        ))

    def produce(s):
        for q in range(FED):
            arrived(s, q)
            stack_arrived(s, q)
            kind, c = PIECES[q]
            if kind == X:
                p_send[s, 0, c] = contract(k_stack[s, 0], x_stack[s, c])
                cross(s, 0, c).start()

        @pl.loop(0, CHUNKS)
        def _(c):
            p_send[s, 1, c] = contract(k_stack[s, 1], x_stack[s, c])
            cross(s, 1, c).start()

    def forward(s):
        @pl.loop(0, CHUNKS)
        def _(c):
            part = contract(k_stack[s, 3, own_terms, :], x_stack[s, c, own_terms, :])
            cross(s, 0, c).wait_recv()
            e_send[s, c] = p_recv[s, 0, c] + part
            deliver(s, c, end).start()

    def own_share(s):
        migrate(len(PIECES), s).wait_recv()

        @pl.loop(0, CHUNKS)
        def _(c):
            result[s, :, chunk(c)] = stiffness(s, c) - contract(k_stack[s, 2], x_stack[s, c])

    def finish(s):
        @pl.loop(0, CHUNKS)
        def _(c):
            cross(s, 1, c).wait_recv()
            result[s, :, chunk(c)] = result[s, :, chunk(c)] - p_recv[s, 1, c]

    def settle_sent(s):
        for c in range(CHUNKS):
            cross(s, 0, c).wait_send()
            cross(s, 1, c).wait_send()

    @pl.when(is_mid)
    def _():
        for s in range(OWN):
            for kind, n in PIECES:
                stack_piece(s, kind, n)

    @pl.when(even_mid)
    def _():
        for q in range(FED):
            arrived(0, q)
            if q < FAR:
                far(1, q).start()
            stack_arrived(0, q)
        own_share(0)
        produce(1)
        own_share(1)
        for source in range(2):
            for q in range(FAR):
                far(source, q).wait_recv()
                stack_far(source, q)

        @pl.loop(0, CHUNKS)
        def _(c):
            e_send[0, c] = contract(k_stack[0, 3, own_terms, :], x_stack[0, c, own_terms, :]) + contract(kf_stack[0], xf_stack[c])
            deliver(0, c, end).start()

        @pl.loop(0, CHUNKS)
        def _(c):
            result[0, :, chunk(c)] = result[0, :, chunk(c)] - contract(kf_stack[1], xf_stack[c])

        forward(1)
        finish(1)
        for source in range(2):
            for q in range(FAR):
                far(source, q).wait_send()
        settle_sent(1)

    @pl.when(odd_mid)
    def _():
        produce(0)
        own_share(0)
        forward(0)
        produce(1)
        own_share(1)
        finish(0)
        forward(1)
        finish(1)
        settle_sent(0)
        settle_sent(1)

    @pl.when(is_mid)
    def _():
        for s in range(OWN):
            for c in range(CHUNKS):
                deliver(s, c, end).wait_send()

    for s in range(OWN):
        for q in range(len(PIECES) + 1):
            migrate(q, s).wait_send()


def line_body(coupling, interior_solve, boundary_stiffness, migration):
    home, depth, columns = interior_solve.shape
    rows = boundary_stiffness.shape[1]
    width = columns // CHUNKS
    f32, bf16 = jnp.float32, jnp.bfloat16
    k_share, x_share, b_share = (OWN, LINE, depth, rows), (OWN, CHUNKS, depth, width), (OWN, rows, columns)
    pieces = (OWN, CHUNKS, rows, width)
    dma = pltpu.SemaphoreType.DMA
    return pl.pallas_call(
        line_kernel,
        out_shape=pltpu.VMEM(b_share, f32),
        in_specs=[pl.BlockSpec(memory_space=pltpu.SMEM)] + [pl.BlockSpec(memory_space=pl.ANY)] * 3,
        out_specs=pl.BlockSpec(memory_space=pltpu.VMEM),
        scratch_shapes=[
            *[pltpu.VMEM((home, depth, rows), f32)] * LINE,
            *[pltpu.VMEM((home, depth, width), f32)] * CHUNKS,
            pltpu.VMEM((home, rows, columns), f32),
            pltpu.VMEM(k_share, f32),
            pltpu.VMEM(x_share, f32),
            pltpu.VMEM(b_share, f32),
            pltpu.VMEM(k_share, f32),
            pltpu.VMEM(x_share, f32),
            pltpu.VMEM(b_share, f32),
            pltpu.VMEM(k_share, f32),
            pltpu.VMEM(x_share, f32),
            pltpu.VMEM((OWN, LINE - 1, depth, rows), f32),
            pltpu.VMEM(x_share, f32),
            pltpu.VMEM((2, 2, depth, rows), f32),
            pltpu.VMEM((2, CHUNKS, depth, width), f32),
            pltpu.VMEM((OWN, LINE, 6 * depth, rows), bf16),
            pltpu.VMEM((OWN, CHUNKS, 6 * depth, width), bf16),
            pltpu.VMEM((2, 6 * depth, rows), bf16),
            pltpu.VMEM((CHUNKS, 6 * depth, width), bf16),
            pltpu.VMEM((OWN, 2, CHUNKS, rows, width), f32),
            pltpu.VMEM((OWN, 2, CHUNKS, rows, width), f32),
            pltpu.VMEM(pieces, f32),
            pltpu.VMEM(pieces, f32),
            dma((len(PIECES) + 1,)),
            dma((OWN, len(PIECES) + 1)),
            dma((OWN, len(PIECES) + 1)),
            dma((OWN, FED)),
            dma((OWN, FED)),
            dma((2, FAR)),
            dma((2, FAR)),
            dma((OWN, 2, CHUNKS)),
            dma((OWN, 2, CHUNKS)),
            dma((OWN, CHUNKS)),
            dma((OWN, CHUNKS)),
        ],
        compiler_params=pltpu.CompilerParams(
            collective_id=0, has_side_effects=True, vmem_limit_bytes=60 * 1024 * 1024
        ),
    )(migration, jnp.swapaxes(coupling, 1, 2), interior_solve, boundary_stiffness)


def solution(mesh):
    return jax.shard_map(
        line_body if mesh.shape["tile"] == LINE else portable_body,
        mesh=mesh,
        in_specs=(
            P("group", None, "tile"),
            P("group", "tile", None),
            P("group", "tile", None),
            P(),
        ),
        out_specs=P("group", "tile", None),
        check_vma=False,
    )
```

```python
import jax
import jax.numpy as jnp
from jax import lax
from jax.experimental import pallas as pl
from jax.experimental.pallas import tpu as pltpu
from jax.sharding import PartitionSpec as P

OWN = 2


def swapped(array, axis, distance):
    return lax.ppermute(array, axis, [(i, i ^ 1 << distance) for i in range(lax.axis_size(axis))])


def condense(coupling_cols, solve_rows, stiff_rows):
    product = lax.psum_scatter(
        jnp.dot(
            coupling_cols,
            solve_rows,
            precision=lax.Precision.HIGHEST,
            preferred_element_type=jnp.float32,
        ),
        "tile",
        scatter_dimension=0,
        tiled=True,
    )
    return stiff_rows - product


def select_slots(stacked, positions, present):
    chosen = jnp.take(stacked, positions, axis=0)
    shaped = present.reshape((-1,) + (1,) * (stacked.ndim - 1))
    return jnp.where(shaped, chosen, jnp.zeros_like(chosen))


def portable_body(coupling, interior_solve, boundary_stiffness, migration):
    home_count = coupling.shape[0]
    mygroup = lax.axis_index("group")
    partner = jnp.bitwise_xor(mygroup, 1)
    own_plan = lax.dynamic_slice_in_dim(migration, mygroup * home_count, home_count)
    slot_ids = jnp.arange(OWN, dtype=jnp.int32)
    local_ids = jnp.arange(home_count, dtype=jnp.int32)

    def locate(wanted):
        matches = own_plan[None, :] == wanted[:, None]
        positions = jnp.sum(jnp.where(matches, local_ids[None, :], 0), axis=1)
        return (positions, jnp.any(matches, axis=1))

    mine_index, mine_here = locate(mygroup * OWN + slot_ids)
    their_index, their_here = locate(partner * OWN + slot_ids)
    keep_mask = mine_here[:, None, None]
    outgoing = (
        select_slots(coupling, their_index, their_here),
        select_slots(interior_solve, their_index, their_here),
        select_slots(boundary_stiffness, their_index, their_here),
    )
    arrived = swapped((outgoing[0], outgoing[1], outgoing[2]), "group", 0)
    kept_coupling = jnp.where(keep_mask, jnp.take(coupling, mine_index, axis=0), arrived[0])
    kept_solve = jnp.where(keep_mask, jnp.take(interior_solve, mine_index, axis=0), arrived[1])
    kept_stiff = jnp.where(keep_mask, jnp.take(boundary_stiffness, mine_index, axis=0), arrived[2])
    result = jnp.stack(
        [condense(kept_coupling[slot], kept_solve[slot], kept_stiff[slot]) for slot in range(OWN)]
    )
    return result


MESH = pl.DeviceIdType.MESH
LINE = 4
CHUNKS = 4
STRIP = 64
AHEAD = 4
K, X = 0, 1
PIECES = ((K, 0), (X, 0), (K, 1), (X, 1), (X, 2), (X, 3), (K, 2), (K, 3))
K_FAR_END, K_FAR_MID, K_MID, K_END = 0, 2, 6, 7
X_AT = (1, 3, 4, 5)
UNITS = ((0, 0, 3), (0, 1, 3), (0, 2, 3)) + tuple((q, 0, 1) for q in range(1, len(PIECES)))
FED = 7
FAR = 6
LATER_FEEDS = ((0, 2), (2, 2), (4, 2), (6, 1))
LATER_CROSSES = ((0, 2), (2, 1), (3, 1))


def split_into(stack, base, depth, rows, value, order):
    high = value.astype(jnp.bfloat16)
    low = (value - high.astype(jnp.float32)).astype(jnp.bfloat16)
    for place, term in enumerate(order):
        stack[pl.ds(base + place * depth + rows, value.shape[0]), :] = high if term == 0 else low


def contract(left, right):
    return lax.dot_general(left, right, (((0,), (0,)), ((), ())), preferred_element_type=jnp.float32)


def strips(count, body):
    @pl.loop(0, count // STRIP)
    def _(i):
        body(pl.multiple_of(i * STRIP, STRIP))


def line_kernel(plan_hbm, k_hbm, x_hbm, b_hbm, result, plan, *scratch):
    homes, scratch = scratch[: len(UNITS)], scratch[len(UNITS) :]
    (
        b_home, leaving, b_out, coming, b_in, got, from_end, from_far, stack, far_stack,
        p_send, p_recv, e_send, e_recv,
        load_sem, mig_send, mig_recv, em_send, em_recv, far_send, far_recv, mm_send, mm_recv, me_send, me_recv,
    ) = scratch
    home, _, width = homes[0].shape
    depth = got.shape[2]
    rows = b_home.shape[1]
    last = LINE - 1
    g, t = lax.axis_index("group"), lax.axis_index("tile")
    parity = g % 2
    partner = g + 1 - 2 * parity
    side = t // 2
    end, mid = side * last, 1 + side
    far_end, across = last - end, last - mid
    is_end = t == end
    is_mid = t == mid
    even_mid = is_mid & (parity == 0)
    odd_mid = is_mid & (parity == 1)

    def chunk(index):
        return pl.ds(pl.multiple_of(index * width, width), width)

    def part(u):
        q, i, n = UNITS[u]
        return q, i * (depth // n), depth // n

    def load(u):
        q, first, count = part(u)
        kind, n = PIECES[q]
        at = chunk(n if kind == X else (far_end, across, mid, end)[n])
        return pltpu.make_async_copy(
            (k_hbm, x_hbm)[kind].at[:, pl.ds(first, count), at], homes[u], load_sem.at[u % AHEAD]
        )

    b_load = pltpu.make_async_copy(b_hbm, b_home, load_sem.at[AHEAD])
    plan_load = pltpu.make_async_copy(plan_hbm, plan, load_sem.at[AHEAD + 1])
    plan_load.start()
    for u in range(AHEAD):
        load(u).start()

    barrier = pltpu.get_barrier_semaphore()
    pl.semaphore_signal(barrier, inc=1, device_id=(partner, t), device_id_type=MESH)

    @pl.when(is_mid)
    def _():
        pl.semaphore_signal(barrier, inc=1, device_id=(g, across), device_id_type=MESH)
        pl.semaphore_signal(barrier, inc=1, device_id=(g, end), device_id_type=MESH)

    plan_load.wait()

    def find(wanted):
        index, here = jnp.int32(0), jnp.int32(0)
        for j in range(home):
            hit = plan[g * home + j] == wanted
            index, here = jnp.where(hit, j, index), jnp.where(hit, 1, here)
        return index, here > 0

    mine = [find(g * OWN + s) for s in range(OWN)]
    theirs = [find(partner * OWN + s) for s in range(OWN)]

    def remote(src, dst, send_sem, recv_sem, to):
        return pltpu.make_async_remote_copy(
            src_ref=src, dst_ref=dst, send_sem=send_sem, recv_sem=recv_sem, device_id=to, device_id_type=MESH
        )

    def migrate(u):
        q, first, count = part(u)
        at = pl.ds(first, count)
        return remote(leaving.at[0, q, at], coming.at[0, q, at], mig_send.at[0], mig_recv.at[u], (partner, t))

    def migrate_later():
        return remote(leaving.at[1], coming.at[1], mig_send.at[0], mig_recv.at[len(UNITS)], (partner, t))

    def migrate_b():
        return remote(b_out, b_in, mig_send.at[1], mig_recv.at[len(UNITS) + 1], (partner, t))

    def feed(q, to):
        return remote(got.at[0, q], from_end.at[0, q], em_send, em_recv.at[q], (g, to))

    def feed_later(i, to):
        at = pl.ds(*LATER_FEEDS[i])
        return remote(got.at[1, at], from_end.at[1, at], em_send, em_recv.at[FED + i], (g, to))

    def far_own(u):
        q, first, count = part(u)
        at = pl.ds(first, count)
        return remote(got.at[0, q, at], from_far.at[0, q, at], far_send, far_recv.at[0], (g, across))

    def far_end_share(q):
        return remote(from_end.at[0, q], from_far.at[1, q], far_send, far_recv.at[1 + q // 4], (g, across))

    def cross_far_end(s, c):
        return remote(
            p_send.at[s, 0, c], p_recv.at[s, 0, c], mm_send.at[s], mm_recv.at[3 + c if s else c // 2], (g, across)
        )

    def cross_far_mid(s, i):
        at = pl.ds(*LATER_CROSSES[i]) if s else pl.ds(0, CHUNKS)
        return remote(
            p_send.at[s, 1, at], p_recv.at[s, 1, at], mm_send.at[s], mm_recv.at[3 + CHUNKS + i if s else 2], (g, across)
        )

    def deliver(s, c):
        return remote(e_send.at[s, c], e_recv.at[s, c], me_send, me_recv.at[s], (g, end))

    def arrival(buffer, sem, source):
        remote(buffer, buffer, sem, sem, source).wait_recv()

    def departed(buffer, sem):
        remote(buffer, buffer, sem, sem, (partner, t)).wait_send()

    def gather(u, s):
        q, first, count = part(u)

        def copy(at):
            leaving[s, q, pl.ds(first + at, STRIP), :] = homes[u][theirs[s][0], pl.ds(at, STRIP), :]

        strips(count, copy)

    def settle(u, s):
        q, first, count = part(u)
        index, here = mine[s]

        def choose(at):
            place = pl.ds(first + at, STRIP)
            got[s, q, place, :] = jnp.where(here, homes[u][index, pl.ds(at, STRIP), :], coming[s, q, place, :])

        strips(count, choose)

    def settle_first(u):
        q, first, count = part(u)
        migrate(u).wait_recv()
        settle(u, 0)
        if q < FED and first + count == depth:
            @pl.when(is_end)
            def _():
                feed(q, mid).start()

        if q < FAR:
            @pl.when(even_mid)
            def _():
                far_own(u).start()

    for u in range(len(UNITS)):
        load(u).wait()
        if u + AHEAD < len(UNITS):
            load(u + AHEAD).start()
        elif u + AHEAD == len(UNITS):
            b_load.start()
        gather(u, 0)
        if u == 0:
            pl.semaphore_wait(barrier, 2)
        migrate(u).start()
        if u > 0:
            settle_first(u - 1)
        gather(u, 1)
    migrate_later().start()
    settle_first(len(UNITS) - 1)

    def stack_piece(s, q, source, base):
        order = ((0, 0, 1), (0, 1, 0))[PIECES[q][0]]
        strips(depth, lambda first: split_into(
            stack.at[s, q], base, depth, first, source[s, q, pl.ds(first, STRIP), :], order
        ))

    def stack_far(source, q):
        order = ((0, 0, 1), (0, 1, 0))[PIECES[q][0]]
        strips(depth, lambda first: split_into(
            far_stack.at[q], 3 * source * depth, depth, first, from_far[source, q, pl.ds(first, STRIP), :], order
        ))

    own_pieces = (K_END,) + X_AT

    @pl.when(is_mid)
    def _():
        for q in range(len(PIECES)):
            stack_piece(0, q, got, 0)

    migrate_later().wait_recv()
    for u in range(len(UNITS)):
        settle(u, 1)

    @pl.when(is_end)
    def _():
        for i in range(len(LATER_FEEDS)):
            feed_later(i, mid).start()

    @pl.when(is_mid)
    def _():
        for q in range(len(PIECES)):
            stack_piece(1, q, got, 0)

    b_load.wait()
    for s in range(OWN):
        def copy(first):
            at = pl.ds(first, STRIP)
            b_out[s, at, :] = b_home[theirs[s][0], at, :]

        strips(rows, copy)
    migrate_b().start()

    def stiffness(s, c):
        index, here = mine[s]
        return jnp.where(here, b_home[index, :, chunk(c)], b_in[s, :, chunk(c)])

    own_terms = pl.ds(0, 3 * depth)

    def x_at(c):
        return jnp.where(c == 0, X_AT[0], c + X_AT[1] - 1)

    @pl.when(is_end)
    def _():
        for s in range(OWN):
            for q in own_pieces:
                stack_piece(s, q, got, 0)
        migrate_b().wait_recv()
        for s in range(OWN):
            @pl.loop(0, CHUNKS)
            def _(c):
                result[s, :, chunk(c)] = stiffness(s, c) - contract(
                    stack[s, K_END, own_terms, :], stack[s, x_at(c), own_terms, :]
                )

        for s in range(OWN):
            arrival(e_recv.at[s], me_recv.at[s], (g, mid))

            @pl.loop(0, CHUNKS)
            def _(c):
                result[s, :, chunk(c)] = result[s, :, chunk(c)] - e_recv[s, c]

        departed(got.at[:, pl.ds(0, FED)], em_send)

    def arrived(s, q):
        if s == 0:
            arrival(from_end.at[0, q], em_recv.at[q], (g, end))
        else:
            for i, (first, count) in enumerate(LATER_FEEDS):
                if first == q:
                    arrival(from_end.at[1, pl.ds(first, count)], em_recv.at[FED + i], (g, end))

    def produce(s, beside=None):
        for q in range(FED):
            arrived(s, q)
            stack_piece(s, q, from_end, 3 * depth)
            kind, c = PIECES[q]
            if kind == X:
                p_send[s, 0, c] = contract(stack[s, K_FAR_END], stack[s, q])
                cross_far_end(s, c).start()
            if beside is not None:
                beside(q)

        def far_mid(first, count):
            @pl.loop(first, first + count)
            def _(c):
                p_send[s, 1, c] = contract(stack[s, K_FAR_MID], stack[s, x_at(c)])

        if s == 0:
            far_mid(0, CHUNKS)
            cross_far_mid(0, 0).start()
        else:
            for i, (first, count) in enumerate(LATER_CROSSES):
                far_mid(first, count)
                cross_far_mid(1, i).start()

    def forward(s):
        for c in range(CHUNKS):
            part = contract(stack[s, K_END, own_terms, :], stack[s, X_AT[c], own_terms, :])
            if s:
                cross_far_end(1, c).wait_recv()
            elif c % 2 == 0:
                arrival(p_recv.at[0, 0, pl.ds(c, 2)], mm_recv.at[c // 2], (g, across))
            e_send[s, c] = p_recv[s, 0, c] + part
            deliver(s, c).start()

    def own_share(s):
        @pl.loop(0, CHUNKS)
        def _(c):
            result[s, :, chunk(c)] = stiffness(s, c) - contract(stack[s, K_MID], stack[s, x_at(c)])

    def finish(s):
        def subtract(first, count):
            @pl.loop(first, first + count)
            def _(c):
                result[s, :, chunk(c)] = result[s, :, chunk(c)] - p_recv[s, 1, c]

        if s == 0:
            cross_far_mid(0, 0).wait_recv()
            subtract(0, CHUNKS)
        else:
            for i, (first, count) in enumerate(LATER_CROSSES):
                cross_far_mid(1, i).wait_recv()
                subtract(first, count)

    def far_arrived(q):
        if q == 2:
            arrival(from_far.at[1, pl.ds(0, 4)], far_recv.at[1], (g, across))
            for p in range(4):
                stack_far(1, p)
        elif q == 4:
            arrival(from_far.at[1, pl.ds(4, 2)], far_recv.at[2], (g, across))
            for p in range(4, FAR):
                stack_far(1, p)
        for c in ((), (), (0, 1), (), (2, 3), (), ())[q]:
            e_send[0, c] = contract(stack[0, K_END, own_terms, :], stack[0, X_AT[c], own_terms, :]) + contract(
                far_stack[K_FAR_END], far_stack[X_AT[c]]
            )
            deliver(0, c).start()

    @pl.when(even_mid)
    def _():
        for q in range(FED):
            arrived(0, q)
            if q < FAR:
                far_end_share(q).start()
            stack_piece(0, q, from_end, 3 * depth)
        arrival(from_far.at[0], far_recv.at[0], (g, across))
        for q in range(FAR):
            stack_far(0, q)
        migrate_b().wait_recv()
        own_share(0)
        produce(1, far_arrived)
        own_share(1)

        @pl.loop(0, CHUNKS)
        def _(c):
            result[0, :, chunk(c)] = result[0, :, chunk(c)] - contract(far_stack[K_FAR_MID], far_stack[x_at(c)])

        forward(1)
        finish(1)
        departed(from_far, far_send)

    @pl.when(odd_mid)
    def _():
        produce(0)
        migrate_b().wait_recv()
        own_share(0)
        forward(0)
        produce(1)
        own_share(1)
        finish(0)
        forward(1)
        finish(1)
        departed(p_send.at[0], mm_send.at[0])

    @pl.when(is_mid)
    def _():
        departed(p_send.at[1], mm_send.at[1])
        departed(e_send, me_send)

    departed(leaving, mig_send.at[0])
    departed(b_out, mig_send.at[1])


def line_body(coupling, interior_solve, boundary_stiffness, migration):
    home, depth, columns = interior_solve.shape
    rows = boundary_stiffness.shape[1]
    width = columns // CHUNKS
    f32, bf16 = jnp.float32, jnp.bfloat16
    b_share, share = (OWN, rows, columns), (OWN, len(PIECES), depth, width)
    pieces = (OWN, CHUNKS, rows, width)
    dma = pltpu.SemaphoreType.DMA
    return pl.pallas_call(
        line_kernel,
        out_shape=pltpu.VMEM(b_share, f32),
        in_specs=[pl.BlockSpec(memory_space=pl.ANY)] * 4,
        out_specs=pl.BlockSpec(memory_space=pltpu.VMEM),
        scratch_shapes=[
            pltpu.SMEM(migration.shape, jnp.int32),
            *[pltpu.VMEM((home, depth // n, width), f32) for _, _, n in UNITS],
            pltpu.VMEM((home, rows, columns), f32),
            pltpu.VMEM(share, f32),
            pltpu.VMEM(b_share, f32),
            pltpu.VMEM(share, f32),
            pltpu.VMEM(b_share, f32),
            pltpu.VMEM(share, f32),
            pltpu.VMEM((OWN, FED, depth, width), f32),
            pltpu.VMEM((2, FAR, depth, width), f32),
            pltpu.VMEM((OWN, len(PIECES), 6 * depth, width), bf16),
            pltpu.VMEM((FAR, 6 * depth, width), bf16),
            pltpu.VMEM((OWN, 2, CHUNKS, rows, width), f32),
            pltpu.VMEM((OWN, 2, CHUNKS, rows, width), f32),
            pltpu.VMEM(pieces, f32),
            pltpu.VMEM(pieces, f32),
            dma((AHEAD + 2,)),
            dma((2,)),
            dma((len(UNITS) + 2,)),
            dma,
            dma((FED + len(LATER_FEEDS),)),
            dma,
            dma((3,)),
            dma((OWN,)),
            dma((3 + CHUNKS + len(LATER_CROSSES),)),
            dma,
            dma((OWN,)),
        ],
        compiler_params=pltpu.CompilerParams(
            collective_id=0, has_side_effects=True, vmem_limit_bytes=60 * 1024 * 1024
        ),
    )(migration, jnp.swapaxes(coupling, 1, 2), interior_solve, boundary_stiffness)


def solution(mesh):
    return jax.shard_map(
        line_body if mesh.shape["tile"] == LINE else portable_body,
        mesh=mesh,
        in_specs=(
            P("group", None, "tile"),
            P("group", "tile", None),
            P("group", "tile", None),
            P(),
        ),
        out_specs=P("group", "tile", None),
        check_vma=False,
    )
```

```python
import jax
import jax.numpy as jnp
from jax import lax
from jax.experimental import pallas as pl
from jax.experimental.pallas import tpu as pltpu
from jax.sharding import PartitionSpec as P

OWN = 2


def swapped(array, axis, distance):
    return lax.ppermute(array, axis, [(i, i ^ 1 << distance) for i in range(lax.axis_size(axis))])


def condense(coupling_cols, solve_rows, stiff_rows):
    product = lax.psum_scatter(
        jnp.dot(
            coupling_cols,
            solve_rows,
            precision=lax.Precision.HIGHEST,
            preferred_element_type=jnp.float32,
        ),
        "tile",
        scatter_dimension=0,
        tiled=True,
    )
    return stiff_rows - product


def select_slots(stacked, positions, present):
    chosen = jnp.take(stacked, positions, axis=0)
    shaped = present.reshape((-1,) + (1,) * (stacked.ndim - 1))
    return jnp.where(shaped, chosen, jnp.zeros_like(chosen))


def portable_body(coupling, interior_solve, boundary_stiffness, migration):
    home_count = coupling.shape[0]
    mygroup = lax.axis_index("group")
    partner = jnp.bitwise_xor(mygroup, 1)
    own_plan = lax.dynamic_slice_in_dim(migration, mygroup * home_count, home_count)
    slot_ids = jnp.arange(OWN, dtype=jnp.int32)
    local_ids = jnp.arange(home_count, dtype=jnp.int32)

    def locate(wanted):
        matches = own_plan[None, :] == wanted[:, None]
        positions = jnp.sum(jnp.where(matches, local_ids[None, :], 0), axis=1)
        return (positions, jnp.any(matches, axis=1))

    mine_index, mine_here = locate(mygroup * OWN + slot_ids)
    their_index, their_here = locate(partner * OWN + slot_ids)
    keep_mask = mine_here[:, None, None]
    outgoing = (
        select_slots(coupling, their_index, their_here),
        select_slots(interior_solve, their_index, their_here),
        select_slots(boundary_stiffness, their_index, their_here),
    )
    arrived = swapped((outgoing[0], outgoing[1], outgoing[2]), "group", 0)
    kept_coupling = jnp.where(keep_mask, jnp.take(coupling, mine_index, axis=0), arrived[0])
    kept_solve = jnp.where(keep_mask, jnp.take(interior_solve, mine_index, axis=0), arrived[1])
    kept_stiff = jnp.where(keep_mask, jnp.take(boundary_stiffness, mine_index, axis=0), arrived[2])
    result = jnp.stack(
        [condense(kept_coupling[slot], kept_solve[slot], kept_stiff[slot]) for slot in range(OWN)]
    )
    return result


MESH = pl.DeviceIdType.MESH
LINE = 4
CHUNKS = 4
STRIP = 64
AHEAD = 4
LAG = 2
K, X = 0, 1
PIECES = ((K, 0), (X, 0), (K, 1), (X, 1), (X, 2), (X, 3), (K, 2), (K, 3))
K_FAR_END, K_FAR_MID, K_MID, K_END = 0, 2, 6, 7
X_AT = (1, 3, 4, 5)
UNITS = ((0, 0, 1), (0, 1, 2), (0, 3, 3)) + tuple((q, 0, 6) for q in range(1, len(PIECES)))
GROUPS = ((0,), (1,), (2,), (3,), (4,), (5, 6, 7), (8, 9))
FED = 7
FAR = 6
LATER_FEEDS = ((0, 2), (2, 2), (4, 2), (6, 1))
CROSSES = (((0, 1), (1, 3)), ((0, 1), (1, 2), (3, 1)))


def split_into(stack, base, depth, rows, value, order):
    high = value.astype(jnp.bfloat16)
    low = (value - high.astype(jnp.float32)).astype(jnp.bfloat16)
    for place, term in enumerate(order):
        stack[pl.ds(base + place * depth + rows, value.shape[0]), :] = high if term == 0 else low


def contract(left, right):
    return lax.dot_general(left, right, (((0,), (0,)), ((), ())), preferred_element_type=jnp.float32)


def strips(count, body):
    strip = STRIP if count % STRIP == 0 else STRIP // 2

    @pl.loop(0, count // strip)
    def _(i):
        first = pl.multiple_of(i * strip, strip)
        body(first, pl.ds(first, strip))


def line_kernel(plan_hbm, k_hbm, x_hbm, b_hbm, result, plan, *scratch):
    homes, scratch = scratch[: len(UNITS)], scratch[len(UNITS) :]
    (
        b_home, leaving, b_out, coming, b_in, got, from_end, from_far, stack, far_stack,
        p_send, p_recv, e_send, e_recv,
        mm_send, mm_recv, me_send, me_recv,
    ) = scratch
    home, _, width = homes[0].shape
    depth = got.shape[2]
    rows = b_home.shape[1]
    last = LINE - 1
    g, t = lax.axis_index("group"), lax.axis_index("tile")
    parity = g % 2
    partner = g + 1 - 2 * parity
    side = t // 2
    end, mid = side * last, 1 + side
    far_end, across = last - end, last - mid
    is_end = t == end
    is_mid = t == mid
    even_mid = is_mid & (parity == 0)
    odd_mid = is_mid & (parity == 1)

    def chunk(index):
        return pl.ds(pl.multiple_of(index * width, width), width)

    def remote(src, dst, send_sem, recv_sem, to):
        return pltpu.make_async_remote_copy(
            src_ref=src, dst_ref=dst, send_sem=send_sem, recv_sem=recv_sem, device_id=to, device_id_type=MESH
        )

    def cross_far_end(s, first, count):
        at = pl.ds(first, count)
        return remote(
            p_send.at[s, 0, at], p_recv.at[s, 0, at], mm_send.at[s], mm_recv.at[2 * s + first // 2], (g, across)
        )

    def cross_far_mid(s, i):
        at = pl.ds(*CROSSES[s][i])
        return remote(
            p_send.at[s, 1, at], p_recv.at[s, 1, at], mm_send.at[s], mm_recv.at[2 * OWN + (1 + i if s else 0)], (g, across)
        )

    def deliver(s, half):
        at = pl.ds(2 * half, 2)
        return remote(e_send.at[s, at], e_recv.at[s, at], me_send, me_recv, (g, end))

    def arrival(buffer, sem, source):
        remote(buffer, buffer, sem, sem, source).wait_recv()

    def departed(buffer, sem):
        remote(buffer, buffer, sem, sem, (partner, t)).wait_send()

    own_terms = pl.ds(0, 3 * depth)

    def x_at(c):
        return jnp.where(c == 0, X_AT[0], c + X_AT[1] - 1)

    def forward(s):
        for half in range(2):
            at = pl.ds(2 * half, 2)
            for c in (2 * half, 2 * half + 1):
                e_send[s, c] = contract(stack[s, K_END, own_terms, :], stack[s, X_AT[c], own_terms, :])
            arrival(p_recv.at[s, 0, at], mm_recv.at[2 * s + half], (g, across))
            for c in (2 * half, 2 * half + 1):
                e_send[s, c] = e_send[s, c] + p_recv[s, 0, c]
            deliver(s, half).start()

    def finish(s):
        def subtract(first, count):
            @pl.loop(first, first + count)
            def _(c):
                result[s, :, chunk(c)] = result[s, :, chunk(c)] - p_recv[s, 1, c]

        if s == 0:
            arrival(p_recv.at[0, 1], mm_recv.at[2 * OWN], (g, across))
            subtract(0, CHUNKS)
        else:
            for i, (first, count) in enumerate(CROSSES[1]):
                cross_far_mid(1, i).wait_recv()
                subtract(first, count)

    def first_phase(load_sem, mig_send, mig_recv, em_send, em_recv, far_send, far_recv):
        def part(u):
            q, first, count = UNITS[u]
            return q, first * (depth // 6), count * (depth // 6)

        def span(group):
            units = [part(u) for u in group]
            if len(group) == 1:
                q, first, count = units[0]
                return q, pl.ds(first, count)
            return pl.ds(units[0][0], len(group)), pl.ds(0, depth)

        def load(u, which=slice(None)):
            q, first, count = part(u)
            kind, n = PIECES[q]
            at = chunk(n if kind == X else (far_end, across, mid, end)[n])
            return pltpu.make_async_copy(
                (k_hbm, x_hbm)[kind].at[which, pl.ds(first, count), at], homes[u].at[which], load_sem.at[u % AHEAD]
            )

        b_load = pltpu.make_async_copy(b_hbm, b_home, load_sem.at[AHEAD])
        plan_load = pltpu.make_async_copy(plan_hbm, plan, load_sem.at[AHEAD + 1])
        plan_load.start()
        for j in range(home):
            load(0, pl.ds(j, 1)).start()
        for u in range(1, AHEAD):
            load(u).start()

        barrier = pltpu.get_barrier_semaphore()
        pl.semaphore_signal(barrier, inc=1, device_id=(partner, t), device_id_type=MESH)

        @pl.when(is_mid)
        def _():
            pl.semaphore_signal(barrier, inc=1, device_id=(g, across), device_id_type=MESH)
            pl.semaphore_signal(barrier, inc=1, device_id=(g, end), device_id_type=MESH)

        plan_load.wait()

        def find(wanted):
            index, here = jnp.int32(0), jnp.int32(0)
            for j in range(home):
                hit = plan[g * home + j] == wanted
                index, here = jnp.where(hit, j, index), jnp.where(hit, 1, here)
            return index, here > 0

        mine = [find(g * OWN + s) for s in range(OWN)]
        theirs = [find(partner * OWN + s) for s in range(OWN)]

        def migrate(i):
            q, at = span(GROUPS[i])
            return remote(leaving.at[0, q, at], coming.at[0, q, at], mig_send.at[0], mig_recv.at[i], (partner, t))

        def migrate_later():
            return remote(leaving.at[1], coming.at[1], mig_send.at[0], mig_recv.at[len(GROUPS)], (partner, t))

        def migrate_b():
            return remote(b_out, b_in, mig_send.at[1], mig_recv.at[len(GROUPS) + 1], (partner, t))

        def feed(q, to):
            return remote(got.at[0, q], from_end.at[0, q], em_send, em_recv.at[q], (g, to))

        def feed_later(i, to):
            at = pl.ds(*LATER_FEEDS[i])
            return remote(got.at[1, at], from_end.at[1, at], em_send, em_recv.at[FED + i], (g, to))

        def far_own(i):
            q, at = span(GROUPS[i])
            return remote(got.at[0, q, at], from_far.at[0, q, at], far_send, far_recv.at[0], (g, across))

        def far_end_share(q):
            return remote(from_end.at[0, q], from_far.at[1, q], far_send, far_recv.at[1 + q // 4], (g, across))

        def gather(u, s):
            q, first, count = part(u)

            def copy(at, rows_at):
                leaving[s, q, pl.ds(first + at, rows_at.size), :] = homes[u][theirs[s][0], rows_at, :]

            strips(count, copy)

        def settle(u, s):
            q, first, count = part(u)
            index, here = mine[s]

            def choose(at, rows_at):
                place = pl.ds(first + at, rows_at.size)
                got[s, q, place, :] = jnp.where(here, homes[u][index, rows_at, :], coming[s, q, place, :])

            strips(count, choose)

        def settle_first(i):
            migrate(i).wait_recv()
            for u in GROUPS[i]:
                q, first, count = part(u)
                settle(u, 0)
                if q < FED and first + count == depth:
                    @pl.when(is_end)
                    def _():
                        feed(q, mid).start()

            if part(GROUPS[i][0])[0] < FAR:
                @pl.when(even_mid)
                def _():
                    far_own(i).start()

        for i, group in enumerate(GROUPS):
            for u in group:
                load(u).wait()
                if u + AHEAD < len(UNITS):
                    load(u + AHEAD).start()
                elif u + AHEAD == len(UNITS):
                    b_load.start()
                gather(u, 0)
            if i == 0:
                pl.semaphore_wait(barrier, 2)
            migrate(i).start()
            if i >= LAG:
                settle_first(i - LAG)
            for u in group:
                gather(u, 1)
        migrate_later().start()
        for i in range(len(GROUPS) - LAG, len(GROUPS)):
            settle_first(i)

        def stack_piece(s, q, source, base):
            order = ((0, 0, 1), (0, 1, 0))[PIECES[q][0]]
            strips(depth, lambda first, at: split_into(stack.at[s, q], base, depth, first, source[s, q, at, :], order))

        def stack_far(source, q):
            order = ((0, 0, 1), (0, 1, 0))[PIECES[q][0]]
            strips(depth, lambda first, at: split_into(
                far_stack.at[q], 3 * source * depth, depth, first, from_far[source, q, at, :], order
            ))

        own_pieces = (K_END,) + X_AT

        @pl.when(is_mid)
        def _():
            for q in range(len(PIECES)):
                stack_piece(0, q, got, 0)

        migrate_later().wait_recv()
        for u in range(len(UNITS)):
            settle(u, 1)

        @pl.when(is_end)
        def _():
            for i in range(len(LATER_FEEDS)):
                feed_later(i, mid).start()

        @pl.when(is_mid)
        def _():
            for q in range(len(PIECES)):
                stack_piece(1, q, got, 0)

        b_load.wait()
        for s in range(OWN):
            def copy(_, at):
                b_out[s, at, :] = b_home[theirs[s][0], at, :]

            strips(rows, copy)
        migrate_b().start()

        def stiffness(s, c):
            index, here = mine[s]
            return jnp.where(here, b_home[index, :, chunk(c)], b_in[s, :, chunk(c)])

        @pl.when(is_end)
        def _():
            for s in range(OWN):
                for q in own_pieces:
                    stack_piece(s, q, got, 0)
            migrate_b().wait_recv()
            for s in range(OWN):
                @pl.loop(0, CHUNKS)
                def _(c):
                    result[s, :, chunk(c)] = stiffness(s, c) - contract(
                        stack[s, K_END, own_terms, :], stack[s, x_at(c), own_terms, :]
                    )

            departed(got.at[:, pl.ds(0, FED)], em_send)

        def arrived(s, q):
            if s == 0:
                arrival(from_end.at[0, q], em_recv.at[q], (g, end))
            else:
                for i, (first, count) in enumerate(LATER_FEEDS):
                    if first == q:
                        arrival(from_end.at[1, pl.ds(first, count)], em_recv.at[FED + i], (g, end))

        def produce(s, beside=None):
            early = beside is None

            def far_mid(i):
                first, count = CROSSES[s][i]

                @pl.loop(first, first + count)
                def _(c):
                    p_send[s, 1, c] = contract(stack[s, K_FAR_MID], stack[s, x_at(c)])

                cross_far_mid(s, i).start()

            for q in range(FED):
                arrived(s, q)
                stack_piece(s, q, from_end, 3 * depth)
                kind, c = PIECES[q]
                if kind == X:
                    p_send[s, 0, c] = contract(stack[s, K_FAR_END], stack[s, q])
                    if s == 0 or c < 2:
                        cross_far_end(s, c, 1).start()
                    elif c == 3:
                        cross_far_end(s, 2, 2).start()
                if early and q == (3 if s else 2):
                    far_mid(0)
                if beside is not None:
                    beside(q)
            for i in range(int(early), len(CROSSES[s])):
                far_mid(i)

        def own_share(s):
            @pl.loop(0, CHUNKS)
            def _(c):
                result[s, :, chunk(c)] = stiffness(s, c) - contract(stack[s, K_MID], stack[s, x_at(c)])

        def far_arrived(q):
            if q == 2:
                arrival(from_far.at[1, pl.ds(0, 4)], far_recv.at[1], (g, across))
                for p in range(4):
                    stack_far(1, p)
            elif q == 4:
                arrival(from_far.at[1, pl.ds(4, 2)], far_recv.at[2], (g, across))
                for p in range(4, FAR):
                    stack_far(1, p)
            for c in ((), (), (0, 1), (), (2, 3), (), ())[q]:
                e_send[0, c] = contract(stack[0, K_END, own_terms, :], stack[0, X_AT[c], own_terms, :]) + contract(
                    far_stack[K_FAR_END], far_stack[X_AT[c]]
                )
                if c % 2:
                    deliver(0, c // 2).start()

        @pl.when(even_mid)
        def _():
            for q in range(FED):
                arrived(0, q)
                if q < FAR:
                    far_end_share(q).start()
                stack_piece(0, q, from_end, 3 * depth)
            arrival(from_far.at[0], far_recv.at[0], (g, across))
            for q in range(FAR):
                stack_far(0, q)
            migrate_b().wait_recv()
            own_share(0)
            produce(1, far_arrived)
            own_share(1)

            @pl.loop(0, CHUNKS)
            def _(c):
                result[0, :, chunk(c)] = result[0, :, chunk(c)] - contract(far_stack[K_FAR_MID], far_stack[x_at(c)])

            departed(from_far, far_send)

        @pl.when(odd_mid)
        def _():
            produce(0)
            migrate_b().wait_recv()
            own_share(0)
            forward(0)
            produce(1)
            own_share(1)
            finish(0)
            departed(p_send.at[0], mm_send.at[0])

        departed(leaving, mig_send.at[0])
        departed(b_out, mig_send.at[1])
    dma = pltpu.SemaphoreType.DMA
    pl.run_scoped(
        first_phase, dma((AHEAD + 2,)), dma((2,)), dma((len(GROUPS) + 2,)), dma, dma((FED + len(LATER_FEEDS),)), dma, dma((3,))
    )

    @pl.when(is_end)
    def _():
        arrival(e_recv, me_recv, (g, mid))
        for s in range(OWN):
            @pl.loop(0, CHUNKS)
            def _(c):
                result[s, :, chunk(c)] = result[s, :, chunk(c)] - e_recv[s, c]


    @pl.when(is_mid)
    def _():
        forward(1)
        finish(1)
        departed(p_send.at[1], mm_send.at[1])
        departed(e_send, me_send)


def line_body(coupling, interior_solve, boundary_stiffness, migration):
    home, depth, columns = interior_solve.shape
    rows = boundary_stiffness.shape[1]
    width = columns // CHUNKS
    f32, bf16 = jnp.float32, jnp.bfloat16
    b_share, share = (OWN, rows, columns), (OWN, len(PIECES), depth, width)
    pieces = (OWN, CHUNKS, rows, width)
    dma = pltpu.SemaphoreType.DMA
    return pl.pallas_call(
        line_kernel,
        out_shape=pltpu.VMEM(b_share, f32),
        in_specs=[pl.BlockSpec(memory_space=pl.ANY)] * 4,
        out_specs=pl.BlockSpec(memory_space=pltpu.VMEM),
        scratch_shapes=[
            pltpu.SMEM(migration.shape, jnp.int32),
            *[pltpu.VMEM((home, depth // 6 * n, width), f32) for _, _, n in UNITS],
            pltpu.VMEM((home, rows, columns), f32),
            pltpu.VMEM(share, f32),
            pltpu.VMEM(b_share, f32),
            pltpu.VMEM(share, f32),
            pltpu.VMEM(b_share, f32),
            pltpu.VMEM(share, f32),
            pltpu.VMEM((OWN, FED, depth, width), f32),
            pltpu.VMEM((2, FAR, depth, width), f32),
            pltpu.VMEM((OWN, len(PIECES), 6 * depth, width), bf16),
            pltpu.VMEM((FAR, 6 * depth, width), bf16),
            pltpu.VMEM((OWN, 2, CHUNKS, rows, width), f32),
            pltpu.VMEM((OWN, 2, CHUNKS, rows, width), f32),
            pltpu.VMEM(pieces, f32),
            pltpu.VMEM(pieces, f32),
            dma((OWN,)),
            dma((2 * OWN + 1 + len(CROSSES[1]),)),
            dma,
            dma,
        ],
        compiler_params=pltpu.CompilerParams(
            collective_id=0, has_side_effects=True, vmem_limit_bytes=60 * 1024 * 1024
        ),
    )(migration, jnp.swapaxes(coupling, 1, 2), interior_solve, boundary_stiffness)


def solution(mesh):
    return jax.shard_map(
        line_body if mesh.shape["tile"] == LINE else portable_body,
        mesh=mesh,
        in_specs=(
            P("group", None, "tile"),
            P("group", "tile", None),
            P("group", "tile", None),
            P(),
        ),
        out_specs=P("group", "tile", None),
        check_vma=False,
    )
```

```python
import jax
import jax.numpy as jnp
from jax import lax
from jax.experimental import pallas as pl
from jax.experimental.pallas import tpu as pltpu
from jax.sharding import PartitionSpec as P

OWN = 2


def swapped(array, axis, distance):
    return lax.ppermute(array, axis, [(i, i ^ 1 << distance) for i in range(lax.axis_size(axis))])


def condense(coupling_cols, solve_rows, stiff_rows):
    product = lax.psum_scatter(
        jnp.dot(
            coupling_cols,
            solve_rows,
            precision=lax.Precision.HIGHEST,
            preferred_element_type=jnp.float32,
        ),
        "tile",
        scatter_dimension=0,
        tiled=True,
    )
    return stiff_rows - product


def select_slots(stacked, positions, present):
    chosen = jnp.take(stacked, positions, axis=0)
    shaped = present.reshape((-1,) + (1,) * (stacked.ndim - 1))
    return jnp.where(shaped, chosen, jnp.zeros_like(chosen))


def portable_body(coupling, interior_solve, boundary_stiffness, migration):
    home_count = coupling.shape[0]
    mygroup = lax.axis_index("group")
    partner = jnp.bitwise_xor(mygroup, 1)
    own_plan = lax.dynamic_slice_in_dim(migration, mygroup * home_count, home_count)
    slot_ids = jnp.arange(OWN, dtype=jnp.int32)
    local_ids = jnp.arange(home_count, dtype=jnp.int32)

    def locate(wanted):
        matches = own_plan[None, :] == wanted[:, None]
        positions = jnp.sum(jnp.where(matches, local_ids[None, :], 0), axis=1)
        return (positions, jnp.any(matches, axis=1))

    mine_index, mine_here = locate(mygroup * OWN + slot_ids)
    their_index, their_here = locate(partner * OWN + slot_ids)
    keep_mask = mine_here[:, None, None]
    outgoing = (
        select_slots(coupling, their_index, their_here),
        select_slots(interior_solve, their_index, their_here),
        select_slots(boundary_stiffness, their_index, their_here),
    )
    arrived = swapped((outgoing[0], outgoing[1], outgoing[2]), "group", 0)
    kept_coupling = jnp.where(keep_mask, jnp.take(coupling, mine_index, axis=0), arrived[0])
    kept_solve = jnp.where(keep_mask, jnp.take(interior_solve, mine_index, axis=0), arrived[1])
    kept_stiff = jnp.where(keep_mask, jnp.take(boundary_stiffness, mine_index, axis=0), arrived[2])
    result = jnp.stack(
        [condense(kept_coupling[slot], kept_solve[slot], kept_stiff[slot]) for slot in range(OWN)]
    )
    return result


MESH = pl.DeviceIdType.MESH
LINE = 4
CHUNKS = 4
STRIP = 64
AHEAD = 4
LAG = 2
K, X = 0, 1
PIECES = ((K, 0), (X, 0), (K, 1), (X, 1), (X, 2), (X, 3), (K, 2), (K, 3))
K_FAR_END, K_FAR_MID, K_MID, K_END = 0, 2, 6, 7
X_AT = (1, 3, 4, 5)
UNITS = ((0, 0, 1), (0, 1, 2), (0, 3, 3)) + tuple((q, 0, 6) for q in range(1, len(PIECES)))
GROUPS = ((0,), (1,), (2,), (3,), (4,), (5, 6, 7), (8, 9))
FED = 7
FAR = 6
LATER_FEEDS = ((0, 2), (2, 2), (4, 2), (6, 1))
CROSSES = (((0, 1), (1, 3)), ((0, 1), (1, 2), (3, 1)))


def split_into(stack, base, depth, rows, value, order):
    high = value.astype(jnp.bfloat16)
    low = (value - high.astype(jnp.float32)).astype(jnp.bfloat16)
    for place, term in enumerate(order):
        stack[pl.ds(base + place * depth + rows, value.shape[0]), :] = high if term == 0 else low


def contract(left, right):
    return lax.dot_general(left, right, (((0,), (0,)), ((), ())), preferred_element_type=jnp.float32)


def strips(count, body):
    strip = STRIP if count % STRIP == 0 else STRIP // 2

    @pl.loop(0, count // strip)
    def _(i):
        first = pl.multiple_of(i * strip, strip)
        body(first, pl.ds(first, strip))


def line_kernel(plan_hbm, k_hbm, x_hbm, b_hbm, result, plan, *scratch):
    homes, scratch = scratch[: len(UNITS)], scratch[len(UNITS) :]
    (
        b_home, leaving, b_out, coming, b_in, got, from_end, from_far, stack, far_stack,
        p_send, p_recv, e_send, e_recv,
        mm_send, mm_recv, me_send, me_recv,
    ) = scratch
    home, _, width = homes[0].shape
    depth = got.shape[2]
    rows = b_home.shape[1]
    last = LINE - 1
    g, t = lax.axis_index("group"), lax.axis_index("tile")
    parity = g % 2
    partner = g + 1 - 2 * parity
    side = t // 2
    end, mid = side * last, 1 + side
    far_end, across = last - end, last - mid
    is_end = t == end
    is_mid = t == mid
    even_mid = is_mid & (parity == 0)
    odd_mid = is_mid & (parity == 1)

    def chunk(index):
        return pl.ds(pl.multiple_of(index * width, width), width)

    def remote(src, dst, send_sem, recv_sem, to):
        return pltpu.make_async_remote_copy(
            src_ref=src, dst_ref=dst, send_sem=send_sem, recv_sem=recv_sem, device_id=to, device_id_type=MESH
        )

    def cross_far_end(s, first, count):
        at = pl.ds(first, count)
        return remote(
            p_send.at[s, 0, at], p_recv.at[s, 0, at], crossing[s][0], crossing[s][1].at[first // 2], (g, across)
        )

    def cross_far_mid(s, i):
        at = pl.ds(*CROSSES[s][i])
        return remote(
            p_send.at[s, 1, at], p_recv.at[s, 1, at], crossing[s][0], crossing[s][1].at[2 + (i if s else 0)], (g, across)
        )

    def deliver(s, half):
        at = pl.ds(2 * half, 2)
        return remote(e_send.at[s, at], e_recv.at[s, at], me_send, me_recv, (g, end))

    def arrival(buffer, sem, source):
        remote(buffer, buffer, sem, sem, source).wait_recv()

    def departed(buffer, sem):
        remote(buffer, buffer, sem, sem, (partner, t)).wait_send()

    own_terms = pl.ds(0, 3 * depth)

    def x_at(c):
        return jnp.where(c == 0, X_AT[0], c + X_AT[1] - 1)

    def forward(s):
        for half in range(2):
            at = pl.ds(2 * half, 2)
            for c in (2 * half, 2 * half + 1):
                e_send[s, c] = contract(stack[s, K_END, own_terms, :], stack[s, X_AT[c], own_terms, :])
            arrival(p_recv.at[s, 0, at], crossing[s][1].at[half], (g, across))
            for c in (2 * half, 2 * half + 1):
                e_send[s, c] = e_send[s, c] + p_recv[s, 0, c]
            deliver(s, half).start()

    def finish(s):
        def subtract(first, count):
            @pl.loop(first, first + count)
            def _(c):
                result[s, :, chunk(c)] = result[s, :, chunk(c)] - p_recv[s, 1, c]

        if s == 0:
            arrival(p_recv.at[0, 1], crossing[0][1].at[2], (g, across))
            subtract(0, CHUNKS)
        else:
            for i, (first, count) in enumerate(CROSSES[1]):
                cross_far_mid(1, i).wait_recv()
                subtract(first, count)

    crossing = {1: (mm_send, mm_recv)}

    def first_phase(
        load_sem, mig_send, mig_recv, em_send, em_recv, far_send, far_recv, first_send, first_recv
    ):
        crossing[0] = (first_send, first_recv)

        def part(u):
            q, first, count = UNITS[u]
            return q, first * (depth // 6), count * (depth // 6)

        def span(group):
            units = [part(u) for u in group]
            if len(group) == 1:
                q, first, count = units[0]
                return q, pl.ds(first, count)
            return pl.ds(units[0][0], len(group)), pl.ds(0, depth)

        def load(u, which=slice(None)):
            q, first, count = part(u)
            kind, n = PIECES[q]
            at = chunk(n if kind == X else (far_end, across, mid, end)[n])
            return pltpu.make_async_copy(
                (k_hbm, x_hbm)[kind].at[which, pl.ds(first, count), at], homes[u].at[which], load_sem.at[u % AHEAD]
            )

        b_load = pltpu.make_async_copy(b_hbm, b_home, load_sem.at[AHEAD])
        plan_load = pltpu.make_async_copy(plan_hbm, plan, load_sem.at[AHEAD + 1])
        plan_load.start()
        for j in range(home):
            load(0, pl.ds(j, 1)).start()
        for u in range(1, AHEAD):
            load(u).start()

        barrier = pltpu.get_barrier_semaphore()
        pl.semaphore_signal(barrier, inc=1, device_id=(partner, t), device_id_type=MESH)

        @pl.when(is_mid)
        def _():
            pl.semaphore_signal(barrier, inc=1, device_id=(g, across), device_id_type=MESH)
            pl.semaphore_signal(barrier, inc=1, device_id=(g, end), device_id_type=MESH)

        plan_load.wait()

        def find(wanted):
            index, here = jnp.int32(0), jnp.int32(0)
            for j in range(home):
                hit = plan[g * home + j] == wanted
                index, here = jnp.where(hit, j, index), jnp.where(hit, 1, here)
            return index, here > 0

        mine = [find(g * OWN + s) for s in range(OWN)]
        theirs = [find(partner * OWN + s) for s in range(OWN)]

        def migrate(i):
            q, at = span(GROUPS[i])
            return remote(leaving.at[0, q, at], coming.at[0, q, at], mig_send.at[0], mig_recv.at[i], (partner, t))

        def migrate_later():
            return remote(leaving.at[1], coming.at[1], mig_send.at[0], mig_recv.at[len(GROUPS)], (partner, t))

        def migrate_b():
            return remote(b_out, b_in, mig_send.at[1], mig_recv.at[len(GROUPS) + 1], (partner, t))

        def feed(q, to):
            return remote(got.at[0, q], from_end.at[0, q], em_send, em_recv.at[q], (g, to))

        def feed_later(i, to):
            at = pl.ds(*LATER_FEEDS[i])
            return remote(got.at[1, at], from_end.at[1, at], em_send, em_recv.at[FED + i], (g, to))

        def far_own(i):
            q, at = span(GROUPS[i])
            return remote(got.at[0, q, at], from_far.at[0, q, at], far_send, far_recv.at[0], (g, across))

        def far_end_share(q):
            return remote(from_end.at[0, q], from_far.at[1, q], far_send, far_recv.at[1 + q // 4], (g, across))

        def gather(u, s):
            q, first, count = part(u)

            def copy(at, rows_at):
                leaving[s, q, pl.ds(first + at, rows_at.size), :] = homes[u][theirs[s][0], rows_at, :]

            strips(count, copy)

        def settle(u, s):
            q, first, count = part(u)
            index, here = mine[s]

            def choose(at, rows_at):
                place = pl.ds(first + at, rows_at.size)
                got[s, q, place, :] = jnp.where(here, homes[u][index, rows_at, :], coming[s, q, place, :])

            strips(count, choose)

        def settle_first(i):
            migrate(i).wait_recv()
            for u in GROUPS[i]:
                q, first, count = part(u)
                settle(u, 0)
                if q < FED and first + count == depth:
                    @pl.when(is_end)
                    def _():
                        feed(q, mid).start()

            if part(GROUPS[i][0])[0] < FAR:
                @pl.when(even_mid)
                def _():
                    far_own(i).start()

        for i, group in enumerate(GROUPS):
            for u in group:
                load(u).wait()
                if u + AHEAD < len(UNITS):
                    load(u + AHEAD).start()
                elif u + AHEAD == len(UNITS):
                    b_load.start()
                gather(u, 0)
            if i == 0:
                pl.semaphore_wait(barrier, 2)
            migrate(i).start()
            if i >= LAG:
                settle_first(i - LAG)
            for u in group:
                gather(u, 1)
        migrate_later().start()
        for i in range(len(GROUPS) - LAG, len(GROUPS)):
            settle_first(i)

        def stack_piece(s, q, source, base):
            order = ((0, 0, 1), (0, 1, 0))[PIECES[q][0]]
            strips(depth, lambda first, at: split_into(stack.at[s, q], base, depth, first, source[s, q, at, :], order))

        def stack_far(source, q):
            order = ((0, 0, 1), (0, 1, 0))[PIECES[q][0]]
            strips(depth, lambda first, at: split_into(
                far_stack.at[q], 3 * source * depth, depth, first, from_far[source, q, at, :], order
            ))

        own_pieces = (K_END,) + X_AT

        @pl.when(is_mid)
        def _():
            for q in range(len(PIECES)):
                stack_piece(0, q, got, 0)

        migrate_later().wait_recv()
        for u in range(len(UNITS)):
            settle(u, 1)

        @pl.when(is_end)
        def _():
            for i in range(len(LATER_FEEDS)):
                feed_later(i, mid).start()

        @pl.when(is_mid)
        def _():
            for q in range(len(PIECES)):
                stack_piece(1, q, got, 0)

        b_load.wait()
        for s in range(OWN):
            def copy(_, at):
                b_out[s, at, :] = b_home[theirs[s][0], at, :]

            strips(rows, copy)
        migrate_b().start()

        def stiffness(s, c):
            index, here = mine[s]
            return jnp.where(here, b_home[index, :, chunk(c)], b_in[s, :, chunk(c)])

        @pl.when(is_end)
        def _():
            for s in range(OWN):
                for q in own_pieces:
                    stack_piece(s, q, got, 0)
            migrate_b().wait_recv()
            for s in range(OWN):
                @pl.loop(0, CHUNKS)
                def _(c):
                    result[s, :, chunk(c)] = stiffness(s, c) - contract(
                        stack[s, K_END, own_terms, :], stack[s, x_at(c), own_terms, :]
                    )

            departed(got.at[:, pl.ds(0, FED)], em_send)

        def arrived(s, q):
            if s == 0:
                arrival(from_end.at[0, q], em_recv.at[q], (g, end))
            else:
                for i, (first, count) in enumerate(LATER_FEEDS):
                    if first == q:
                        arrival(from_end.at[1, pl.ds(first, count)], em_recv.at[FED + i], (g, end))

        def produce(s, beside=None):
            def far_mid(i):
                first, count = CROSSES[s][i]

                @pl.loop(first, first + count)
                def _(c):
                    p_send[s, 1, c] = contract(stack[s, K_FAR_MID], stack[s, x_at(c)])

                cross_far_mid(s, i).start()

            for q in range(FED):
                arrived(s, q)
                stack_piece(s, q, from_end, 3 * depth)
                kind, c = PIECES[q]
                if kind == X:
                    p_send[s, 0, c] = contract(stack[s, K_FAR_END], stack[s, q])
                    if s == 0 or c < 2:
                        cross_far_end(s, c, 1).start()
                    elif c == 3:
                        cross_far_end(s, 2, 2).start()
                if q == (3 if s else 2):
                    far_mid(0)
                if beside is not None:
                    beside(q)
            for i in range(1, len(CROSSES[s])):
                far_mid(i)

        def own_share(s):
            @pl.loop(0, CHUNKS)
            def _(c):
                result[s, :, chunk(c)] = stiffness(s, c) - contract(stack[s, K_MID], stack[s, x_at(c)])

        def far_arrived(q):
            if q == 2:
                arrival(from_far.at[1, pl.ds(0, 4)], far_recv.at[1], (g, across))
                for p in range(4):
                    stack_far(1, p)
            elif q == 4:
                arrival(from_far.at[1, pl.ds(4, 2)], far_recv.at[2], (g, across))
                for p in range(4, FAR):
                    stack_far(1, p)
            for c in ((), (), (0, 1), (), (2, 3), (), ())[q]:
                e_send[0, c] = contract(stack[0, K_END, own_terms, :], stack[0, X_AT[c], own_terms, :]) + contract(
                    far_stack[K_FAR_END], far_stack[X_AT[c]]
                )
                if c % 2:
                    deliver(0, c // 2).start()

        @pl.when(even_mid)
        def _():
            for q in range(FED):
                arrived(0, q)
                if q < FAR:
                    far_end_share(q).start()
                stack_piece(0, q, from_end, 3 * depth)
            arrival(from_far.at[0], far_recv.at[0], (g, across))
            for q in range(FAR):
                stack_far(0, q)
            migrate_b().wait_recv()
            own_share(0)
            produce(1, far_arrived)
            own_share(1)

            @pl.loop(0, CHUNKS)
            def _(c):
                result[0, :, chunk(c)] = result[0, :, chunk(c)] - contract(far_stack[K_FAR_MID], far_stack[x_at(c)])

            departed(from_far, far_send)

        @pl.when(odd_mid)
        def _():
            produce(0)
            migrate_b().wait_recv()
            own_share(0)
            forward(0)
            produce(1)
            own_share(1)
            finish(0)
            departed(p_send.at[0], first_send)

        departed(leaving, mig_send.at[0])
        departed(b_out, mig_send.at[1])
    dma = pltpu.SemaphoreType.DMA
    pl.run_scoped(
        first_phase, dma((AHEAD + 2,)), dma((2,)), dma((len(GROUPS) + 2,)), dma, dma((FED + len(LATER_FEEDS),)),
        dma, dma((3,)), dma, dma((3,)),
    )

    @pl.when(is_end)
    def _():
        arrival(e_recv, me_recv, (g, mid))
        for s in range(OWN):
            @pl.loop(0, CHUNKS)
            def _(c):
                result[s, :, chunk(c)] = result[s, :, chunk(c)] - e_recv[s, c]


    @pl.when(is_mid)
    def _():
        forward(1)
        finish(1)
        departed(p_send.at[1], mm_send)
        departed(e_send, me_send)


def line_body(coupling, interior_solve, boundary_stiffness, migration):
    home, depth, columns = interior_solve.shape
    rows = boundary_stiffness.shape[1]
    width = columns // CHUNKS
    f32, bf16 = jnp.float32, jnp.bfloat16
    b_share, share = (OWN, rows, columns), (OWN, len(PIECES), depth, width)
    pieces = (OWN, CHUNKS, rows, width)
    dma = pltpu.SemaphoreType.DMA
    return pl.pallas_call(
        line_kernel,
        out_shape=pltpu.VMEM(b_share, f32),
        in_specs=[pl.BlockSpec(memory_space=pl.ANY)] * 4,
        out_specs=pl.BlockSpec(memory_space=pltpu.VMEM),
        scratch_shapes=[
            pltpu.SMEM(migration.shape, jnp.int32),
            *[pltpu.VMEM((home, depth // 6 * n, width), f32) for _, _, n in UNITS],
            pltpu.VMEM((home, rows, columns), f32),
            pltpu.VMEM(share, f32),
            pltpu.VMEM(b_share, f32),
            pltpu.VMEM(share, f32),
            pltpu.VMEM(b_share, f32),
            pltpu.VMEM(share, f32),
            pltpu.VMEM((OWN, FED, depth, width), f32),
            pltpu.VMEM((2, FAR, depth, width), f32),
            pltpu.VMEM((OWN, len(PIECES), 6 * depth, width), bf16),
            pltpu.VMEM((FAR, 6 * depth, width), bf16),
            pltpu.VMEM((OWN, 2, CHUNKS, rows, width), f32),
            pltpu.VMEM((OWN, 2, CHUNKS, rows, width), f32),
            pltpu.VMEM(pieces, f32),
            pltpu.VMEM(pieces, f32),
            dma,
            dma((2 + len(CROSSES[1]),)),
            dma,
            dma,
        ],
        compiler_params=pltpu.CompilerParams(
            collective_id=0, has_side_effects=True, vmem_limit_bytes=60 * 1024 * 1024
        ),
    )(migration, jnp.swapaxes(coupling, 1, 2), interior_solve, boundary_stiffness)


def solution(mesh):
    return jax.shard_map(
        line_body if mesh.shape["tile"] == LINE else portable_body,
        mesh=mesh,
        in_specs=(
            P("group", None, "tile"),
            P("group", "tile", None),
            P("group", "tile", None),
            P(),
        ),
        out_specs=P("group", "tile", None),
        check_vma=False,
    )
```

```python
import jax
import jax.numpy as jnp
from jax import lax
from jax.experimental import pallas as pl
from jax.experimental.pallas import tpu as pltpu
from jax.sharding import PartitionSpec as P

OWN = 2


def swapped(array, axis, distance):
    return lax.ppermute(array, axis, [(i, i ^ 1 << distance) for i in range(lax.axis_size(axis))])


def condense(coupling_cols, solve_rows, stiff_rows):
    product = lax.psum_scatter(
        jnp.dot(
            coupling_cols,
            solve_rows,
            precision=lax.Precision.HIGHEST,
            preferred_element_type=jnp.float32,
        ),
        "tile",
        scatter_dimension=0,
        tiled=True,
    )
    return stiff_rows - product


def select_slots(stacked, positions, present):
    chosen = jnp.take(stacked, positions, axis=0)
    shaped = present.reshape((-1,) + (1,) * (stacked.ndim - 1))
    return jnp.where(shaped, chosen, jnp.zeros_like(chosen))


def portable_body(coupling, interior_solve, boundary_stiffness, migration):
    home_count = coupling.shape[0]
    mygroup = lax.axis_index("group")
    partner = jnp.bitwise_xor(mygroup, 1)
    own_plan = lax.dynamic_slice_in_dim(migration, mygroup * home_count, home_count)
    slot_ids = jnp.arange(OWN, dtype=jnp.int32)
    local_ids = jnp.arange(home_count, dtype=jnp.int32)

    def locate(wanted):
        matches = own_plan[None, :] == wanted[:, None]
        positions = jnp.sum(jnp.where(matches, local_ids[None, :], 0), axis=1)
        return (positions, jnp.any(matches, axis=1))

    mine_index, mine_here = locate(mygroup * OWN + slot_ids)
    their_index, their_here = locate(partner * OWN + slot_ids)
    keep_mask = mine_here[:, None, None]
    outgoing = (
        select_slots(coupling, their_index, their_here),
        select_slots(interior_solve, their_index, their_here),
        select_slots(boundary_stiffness, their_index, their_here),
    )
    arrived = swapped((outgoing[0], outgoing[1], outgoing[2]), "group", 0)
    kept_coupling = jnp.where(keep_mask, jnp.take(coupling, mine_index, axis=0), arrived[0])
    kept_solve = jnp.where(keep_mask, jnp.take(interior_solve, mine_index, axis=0), arrived[1])
    kept_stiff = jnp.where(keep_mask, jnp.take(boundary_stiffness, mine_index, axis=0), arrived[2])
    result = jnp.stack(
        [condense(kept_coupling[slot], kept_solve[slot], kept_stiff[slot]) for slot in range(OWN)]
    )
    return result


MESH = pl.DeviceIdType.MESH
LINE = 4
CHUNKS = 4
STRIP = 64
AHEAD = 5
LAG = 2
K, X = 0, 1
PIECES = ((K, 0), (X, 0), (K, 1), (X, 1), (X, 2), (X, 3), (K, 2), (K, 3))
K_FAR_END, K_FAR_MID, K_MID, K_END = 0, 2, 6, 7
X_AT = (1, 3, 4, 5)
UNITS = ((0, 0, 1), (0, 1, 1), (0, 2, 2), (0, 4, 2)) + tuple((q, 0, 6) for q in range(1, len(PIECES)))
GROUPS = ((0,), (1,), (2,), (3,), (4,), (5,), (6, 7, 8), (9, 10))
TWICE = 1
FAR_SEMS = (0, 0, 1, 1, 2, 2, 2)
FED = 7
FAR = 6
LATER_FEEDS = ((0, 2), (2, 2), (4, 2), (6, 1))
CROSSES = (((0, 1), (1, 3)), ((0, 1), (1, 2), (3, 1)))


def split_into(stack, base, depth, rows, value, order):
    high = value.astype(jnp.bfloat16)
    low = (value - high.astype(jnp.float32)).astype(jnp.bfloat16)
    for place, term in enumerate(order):
        stack[pl.ds(base + place * depth + rows, value.shape[0]), :] = high if term == 0 else low


def contract(left, right):
    return lax.dot_general(left, right, (((0,), (0,)), ((), ())), preferred_element_type=jnp.float32)


def strips(count, body):
    strip = STRIP if count % STRIP == 0 else STRIP // 2

    @pl.loop(0, count // strip)
    def _(i):
        first = pl.multiple_of(i * strip, strip)
        body(first, pl.ds(first, strip))


def line_kernel(plan_hbm, k_hbm, x_hbm, b_hbm, result, plan, *scratch):
    homes, scratch = scratch[: len(UNITS)], scratch[len(UNITS) :]
    (
        b_home, leaving, b_out, coming, b_in, got, from_end, from_far, own_try, far_tries, stack, far_stack,
        p_send, p_recv, e_send, e_recv,
        mm_send, mm_recv, me_send, me_recv,
    ) = scratch
    home, _, width = homes[0].shape
    depth = got.shape[2]
    rows = b_home.shape[1]
    last = LINE - 1
    g, t = lax.axis_index("group"), lax.axis_index("tile")
    parity = g % 2
    partner = g + 1 - 2 * parity
    side = t // 2
    end, mid = side * last, 1 + side
    far_end, across = last - end, last - mid
    is_end = t == end
    is_mid = t == mid
    factor_mid = is_mid & (parity == 1)
    other_mid = is_mid & (parity == 0)

    def chunk(index):
        return pl.ds(pl.multiple_of(index * width, width), width)

    def remote(src, dst, send_sem, recv_sem, to):
        return pltpu.make_async_remote_copy(
            src_ref=src, dst_ref=dst, send_sem=send_sem, recv_sem=recv_sem, device_id=to, device_id_type=MESH
        )

    def cross_far_end(s, first, count):
        at = pl.ds(first, count)
        return remote(
            p_send.at[s, 0, at], p_recv.at[s, 0, at], mm_send.at[s], mm_recv.at[2 * s + first // 2], (g, across)
        )

    def cross_far_mid(s, i):
        at = pl.ds(*CROSSES[s][i])
        return remote(
            p_send.at[s, 1, at], p_recv.at[s, 1, at], mm_send.at[s], mm_recv.at[2 * OWN + (1 + i if s else 0)], (g, across)
        )

    def deliver(s, half):
        at = pl.ds(2 * half, 2)
        return remote(e_send.at[s, at], e_recv.at[s, at], me_send, me_recv, (g, end))

    def arrival(buffer, sem, source):
        remote(buffer, buffer, sem, sem, source).wait_recv()

    def departed(buffer, sem):
        remote(buffer, buffer, sem, sem, (partner, t)).wait_send()

    own_terms = pl.ds(0, 3 * depth)

    def x_at(c):
        return jnp.where(c == 0, X_AT[0], c + X_AT[1] - 1)

    def forward(s):
        for half in range(2):
            at = pl.ds(2 * half, 2)
            for c in (2 * half, 2 * half + 1):
                e_send[s, c] = contract(stack[s, K_END, own_terms, :], stack[s, X_AT[c], own_terms, :])
            arrival(p_recv.at[s, 0, at], mm_recv.at[2 * s + half], (g, across))
            for c in (2 * half, 2 * half + 1):
                e_send[s, c] = e_send[s, c] + p_recv[s, 0, c]
            deliver(s, half).start()

    def finish(s):
        def subtract(first, count):
            @pl.loop(first, first + count)
            def _(c):
                result[s, :, chunk(c)] = result[s, :, chunk(c)] - p_recv[s, 1, c]

        if s == 0:
            arrival(p_recv.at[0, 1], mm_recv.at[2 * OWN], (g, across))
            subtract(0, CHUNKS)
        else:
            for i, (first, count) in enumerate(CROSSES[1]):
                cross_far_mid(1, i).wait_recv()
                subtract(first, count)

    def first_phase(load_sem, mig_send, mig_recv, em_send, em_recv, far_send, far_recv, try_send, try_recv):
        def part(u):
            q, first, count = UNITS[u]
            return q, first * (depth // 6), count * (depth // 6)

        def span(group):
            units = [part(u) for u in group]
            if len(group) == 1:
                q, first, count = units[0]
                return q, pl.ds(first, count)
            return pl.ds(units[0][0], len(group)), pl.ds(0, depth)

        def load(u, which=slice(None)):
            q, first, count = part(u)
            kind, n = PIECES[q]
            at = chunk(n if kind == X else (far_end, across, mid, end)[n])
            return pltpu.make_async_copy(
                (k_hbm, x_hbm)[kind].at[which, pl.ds(first, count), at], homes[u].at[which], load_sem.at[u % AHEAD]
            )

        b_load = pltpu.make_async_copy(b_hbm, b_home, load_sem.at[AHEAD])
        plan_load = pltpu.make_async_copy(plan_hbm, plan, load_sem.at[AHEAD + 1])
        plan_load.start()
        for j in range(home):
            load(0, pl.ds(j, 1)).start()
        for u in range(1, AHEAD):
            load(u).start()

        barrier = pltpu.get_barrier_semaphore()
        pl.semaphore_signal(barrier, inc=1, device_id=(partner, t), device_id_type=MESH)

        @pl.when(is_mid)
        def _():
            pl.semaphore_signal(barrier, inc=1, device_id=(g, across), device_id_type=MESH)
            pl.semaphore_signal(barrier, inc=1, device_id=(g, end), device_id_type=MESH)

        @pl.when(factor_mid)
        def _():
            pl.semaphore_signal(barrier, inc=1, device_id=(partner, across), device_id_type=MESH)

        plan_load.wait()

        def find(wanted):
            index, here = jnp.int32(0), jnp.int32(0)
            for j in range(home):
                hit = plan[g * home + j] == wanted
                index, here = jnp.where(hit, j, index), jnp.where(hit, 1, here)
            return index, here > 0

        mine = [find(g * OWN + s) for s in range(OWN)]
        theirs = [find(partner * OWN + s) for s in range(OWN)]

        def migrate(i):
            q, at = span(GROUPS[i])
            return remote(leaving.at[0, q, at], coming.at[0, q, at], mig_send.at[0], mig_recv.at[i], (partner, t))

        def migrate_later():
            return remote(leaving.at[1], coming.at[1], mig_send.at[0], mig_recv.at[len(GROUPS)], (partner, t))

        def migrate_b():
            return remote(b_out, b_in, mig_send.at[1], mig_recv.at[len(GROUPS) + 1], (partner, t))

        def feed(q, to):
            return remote(got.at[0, q], from_end.at[0, q], em_send, em_recv.at[q], (g, to))

        def feed_later(i, to):
            at = pl.ds(*LATER_FEEDS[i])
            return remote(got.at[1, at], from_end.at[1, at], em_send, em_recv.at[FED + i], (g, to))

        def far_own(i):
            q, at = span(GROUPS[i])
            return remote(got.at[0, q, at], from_far.at[0, q, at], far_send, far_recv.at[FAR_SEMS[i]], (g, across))

        def far_end_share(q):
            return remote(from_end.at[0, q], from_far.at[1, q], far_send, far_recv.at[3 + q // 4], (g, across))

        def gather(u, s):
            q, first, count = part(u)

            def copy(at, rows_at):
                leaving[s, q, pl.ds(first + at, rows_at.size), :] = homes[u][theirs[s][0], rows_at, :]

            strips(count, copy)

        def settle(u, s):
            q, first, count = part(u)
            index, here = mine[s]

            def choose(at, rows_at):
                place = pl.ds(first + at, rows_at.size)
                got[s, q, place, :] = jnp.where(here, homes[u][index, rows_at, :], coming[s, q, place, :])

            strips(count, choose)

        def send_tries():
            q, first, count = part(TWICE)

            @pl.when(factor_mid)
            def _():
                def copy(_, at):
                    own_try[at, :] = homes[TWICE][mine[0][0], at, :]

                strips(count, copy)
                remote(own_try, far_tries.at[0], far_send, try_recv.at[0], (g, across)).start()

            @pl.when(other_mid)
            def _():
                mine_of_partner = leaving.at[0, q, pl.ds(first, count)]
                remote(mine_of_partner, far_tries.at[1], try_send, try_recv.at[1], (partner, across)).start()

        def settle_first(i):
            migrate(i).wait_recv()
            for u in GROUPS[i]:
                q, first, count = part(u)
                settle(u, 0)
                if q < FED and first + count == depth:
                    @pl.when(is_end)
                    def _():
                        feed(q, mid).start()

            if i != TWICE and part(GROUPS[i][0])[0] < FAR:
                @pl.when(factor_mid)
                def _():
                    far_own(i).start()

        for i, group in enumerate(GROUPS):
            for u in group:
                load(u).wait()
                if u + AHEAD < len(UNITS):
                    load(u + AHEAD).start()
                elif u + AHEAD == len(UNITS):
                    b_load.start()
                gather(u, 0)
            if i == 0:
                @pl.when(other_mid)
                def _():
                    pl.semaphore_wait(barrier, 3)

                @pl.when(jnp.logical_not(other_mid))
                def _():
                    pl.semaphore_wait(barrier, 2)

            if i == TWICE:
                send_tries()
            migrate(i).start()
            if i >= LAG:
                settle_first(i - LAG)
            for u in group:
                gather(u, 1)
        migrate_later().start()
        for i in range(len(GROUPS) - LAG, len(GROUPS)):
            settle_first(i)

        def stack_piece(s, q, source, base):
            order = ((0, 0, 1), (0, 1, 0))[PIECES[q][0]]
            strips(depth, lambda first, at: split_into(stack.at[s, q], base, depth, first, source[s, q, at, :], order))

        def stack_far(source, q):
            order = ((0, 0, 1), (0, 1, 0))[PIECES[q][0]]
            strips(depth, lambda first, at: split_into(
                far_stack.at[q], 3 * source * depth, depth, first, from_far[source, q, at, :], order
            ))

        own_pieces = (K_END,) + X_AT

        @pl.when(is_mid)
        def _():
            for q in range(len(PIECES)):
                stack_piece(0, q, got, 0)

        migrate_later().wait_recv()
        for u in range(len(UNITS)):
            settle(u, 1)

        @pl.when(is_end)
        def _():
            for i in range(len(LATER_FEEDS)):
                feed_later(i, mid).start()

        @pl.when(is_mid)
        def _():
            for q in range(len(PIECES)):
                stack_piece(1, q, got, 0)

        b_load.wait()
        for s in range(OWN):
            def copy(_, at):
                b_out[s, at, :] = b_home[theirs[s][0], at, :]

            strips(rows, copy)
        migrate_b().start()

        def stiffness(s, c):
            index, here = mine[s]
            return jnp.where(here, b_home[index, :, chunk(c)], b_in[s, :, chunk(c)])

        @pl.when(is_end)
        def _():
            for s in range(OWN):
                for q in own_pieces:
                    stack_piece(s, q, got, 0)
            migrate_b().wait_recv()
            for s in range(OWN):
                @pl.loop(0, CHUNKS)
                def _(c):
                    result[s, :, chunk(c)] = stiffness(s, c) - contract(
                        stack[s, K_END, own_terms, :], stack[s, x_at(c), own_terms, :]
                    )

            departed(got.at[:, pl.ds(0, FED)], em_send)

        def arrived(s, q):
            if s == 0:
                arrival(from_end.at[0, q], em_recv.at[q], (g, end))
            else:
                for i, (first, count) in enumerate(LATER_FEEDS):
                    if first == q:
                        arrival(from_end.at[1, pl.ds(first, count)], em_recv.at[FED + i], (g, end))

        def produce(s, beside=None):
            early = beside is None

            def far_mid(i):
                first, count = CROSSES[s][i]

                @pl.loop(first, first + count)
                def _(c):
                    p_send[s, 1, c] = contract(stack[s, K_FAR_MID], stack[s, x_at(c)])

                cross_far_mid(s, i).start()

            for q in range(FED):
                arrived(s, q)
                stack_piece(s, q, from_end, 3 * depth)
                kind, c = PIECES[q]
                if kind == X:
                    p_send[s, 0, c] = contract(stack[s, K_FAR_END], stack[s, q])
                    if s == 0 or c < 2:
                        cross_far_end(s, c, 1).start()
                    elif c == 3:
                        cross_far_end(s, 2, 2).start()
                if early and q == (3 if s else 2):
                    far_mid(0)
                if beside is not None:
                    beside(q)
            for i in range(int(early), len(CROSSES[s])):
                far_mid(i)

        def own_share(s):
            @pl.loop(0, CHUNKS)
            def _(c):
                result[s, :, chunk(c)] = stiffness(s, c) - contract(stack[s, K_MID], stack[s, x_at(c)])

        def far_arrived(q):
            if q == 2:
                arrival(from_far.at[1, pl.ds(0, 4)], far_recv.at[3], (g, across))
                for p in range(4):
                    stack_far(1, p)
            elif q == 4:
                arrival(from_far.at[1, pl.ds(4, 2)], far_recv.at[4], (g, across))
                for p in range(4, FAR):
                    stack_far(1, p)
            for c in ((), (), (0, 1), (), (2, 3), (), ())[q]:
                e_send[0, c] = contract(stack[0, K_END, own_terms, :], stack[0, X_AT[c], own_terms, :]) + contract(
                    far_stack[K_FAR_END], far_stack[X_AT[c]]
                )
                if c % 2:
                    deliver(0, c // 2).start()

        @pl.when(factor_mid)
        def _():
            for q in range(FED):
                arrived(0, q)
                if q < FAR:
                    far_end_share(q).start()
                stack_piece(0, q, from_end, 3 * depth)
            arrival(far_tries.at[0], try_recv.at[0], (g, across))
            arrival(far_tries.at[1], try_recv.at[1], (partner, across))
            q, first, count = part(TWICE)
            from_far[0, q, pl.ds(first, count), :] = jnp.where(mine[0][1], far_tries[0], far_tries[1])
            arrival(from_far.at[0, 0, pl.ds(0, first)], far_recv.at[0], (g, across))
            arrival(from_far.at[0, 0, pl.ds(first + count, depth - first - count)], far_recv.at[1], (g, across))
            arrival(from_far.at[0, pl.ds(1, FAR - 1)], far_recv.at[2], (g, across))
            for q in range(FAR):
                stack_far(0, q)
            migrate_b().wait_recv()
            own_share(0)
            produce(1, far_arrived)
            own_share(1)

            @pl.loop(0, CHUNKS)
            def _(c):
                result[0, :, chunk(c)] = result[0, :, chunk(c)] - contract(far_stack[K_FAR_MID], far_stack[x_at(c)])

            departed(from_far, far_send)

        @pl.when(other_mid)
        def _():
            produce(0)
            migrate_b().wait_recv()
            own_share(0)
            forward(0)
            produce(1)
            own_share(1)
            finish(0)
            departed(p_send.at[0], mm_send.at[0])
            departed(far_tries.at[1], try_send)

        departed(leaving, mig_send.at[0])
        departed(b_out, mig_send.at[1])
    dma = pltpu.SemaphoreType.DMA
    pl.run_scoped(
        first_phase, dma((AHEAD + 2,)), dma((2,)), dma((len(GROUPS) + 2,)), dma, dma((FED + len(LATER_FEEDS),)),
        dma, dma((5,)), dma, dma((2,)),
    )

    @pl.when(is_end)
    def _():
        arrival(e_recv, me_recv, (g, mid))
        for s in range(OWN):
            @pl.loop(0, CHUNKS)
            def _(c):
                result[s, :, chunk(c)] = result[s, :, chunk(c)] - e_recv[s, c]


    @pl.when(is_mid)
    def _():
        forward(1)
        finish(1)
        departed(p_send.at[1], mm_send.at[1])
        departed(e_send, me_send)


def line_body(coupling, interior_solve, boundary_stiffness, migration):
    home, depth, columns = interior_solve.shape
    rows = boundary_stiffness.shape[1]
    width = columns // CHUNKS
    f32, bf16 = jnp.float32, jnp.bfloat16
    b_share, share = (OWN, rows, columns), (OWN, len(PIECES), depth, width)
    pieces = (OWN, CHUNKS, rows, width)
    dma = pltpu.SemaphoreType.DMA
    return pl.pallas_call(
        line_kernel,
        out_shape=pltpu.VMEM(b_share, f32),
        in_specs=[pl.BlockSpec(memory_space=pl.ANY)] * 4,
        out_specs=pl.BlockSpec(memory_space=pltpu.VMEM),
        scratch_shapes=[
            pltpu.SMEM(migration.shape, jnp.int32),
            *[pltpu.VMEM((home, depth // 6 * n, width), f32) for _, _, n in UNITS],
            pltpu.VMEM((home, rows, columns), f32),
            pltpu.VMEM(share, f32),
            pltpu.VMEM(b_share, f32),
            pltpu.VMEM(share, f32),
            pltpu.VMEM(b_share, f32),
            pltpu.VMEM(share, f32),
            pltpu.VMEM((OWN, FED, depth, width), f32),
            pltpu.VMEM((2, FAR, depth, width), f32),
            pltpu.VMEM((depth // 6, width), f32),
            pltpu.VMEM((2, depth // 6, width), f32),
            pltpu.VMEM((OWN, len(PIECES), 6 * depth, width), bf16),
            pltpu.VMEM((FAR, 6 * depth, width), bf16),
            pltpu.VMEM((OWN, 2, CHUNKS, rows, width), f32),
            pltpu.VMEM((OWN, 2, CHUNKS, rows, width), f32),
            pltpu.VMEM(pieces, f32),
            pltpu.VMEM(pieces, f32),
            dma((OWN,)),
            dma((2 * OWN + 1 + len(CROSSES[1]),)),
            dma,
            dma,
        ],
        compiler_params=pltpu.CompilerParams(
            collective_id=0, has_side_effects=True, vmem_limit_bytes=60 * 1024 * 1024
        ),
    )(migration, jnp.swapaxes(coupling, 1, 2), interior_solve, boundary_stiffness)


def solution(mesh):
    return jax.shard_map(
        line_body if mesh.shape["tile"] == LINE else portable_body,
        mesh=mesh,
        in_specs=(
            P("group", None, "tile"),
            P("group", "tile", None),
            P("group", "tile", None),
            P(),
        ),
        out_specs=P("group", "tile", None),
        check_vma=False,
    )
```
